1024 devices in a mesh: gz: 8 (over x), gy: 32 (over y_lo, z), gx: 4 (over y_hi, core).
Axes of the slice: x: 8, y: 8 (y_hi: 2, y_lo: 4; y = y_hi * 4 + y_lo), z: 8, core: 2. Of those that a mesh axis runs over, the one named last changes fastest.
Arguments:
- density: float32 [64, 256, 512], P('gz', 'gy', 'gx'), may hold values from 0.3 to 3
- velocity: float32 [3, 64, 256, 512], P(None, 'gz', 'gy', 'gx'), may hold values from -3 to 3
- pressure: float32 [64, 256, 512], P('gz', 'gy', 'gx'), may hold values from 0.3 to 3
- field: float32 [3, 64, 256, 512], P(None, 'gz', 'gy', 'gx'), may hold values from -3 to 3
- corona: int32 [64], replicated, may hold values from 0 to 1, as said below
Outputs:
- conserved: float32 [5, 64, 256, 512], P(None, 'gz', 'gy', 'gx')
- faces_new: float32 [3, 64, 256, 512], P(None, 'gz', 'gy', 'gx')
The draws below stay inside these ranges and needn't reach their ends.
Inputs may be any that keep to these rules, and one draw needn't show every extreme that they name: `corona`: 1 marks a cooled slab; every slab farther from the midplane than a drawn height (one for each half of z) is cooled, and some other slabs are cooled too.
All inputs are finite; a program needn't handle non-finite values.
Results may differ from the reference program's by a relative error of at most 0.00002.
Values sent between devices are 32-bit elements; how exact they have to be, the bound alone decides.
No kernel may reach another device: no remote copies, remote signals or barrier semaphores. Data moves between devices by JAX's collectives and lax.ppermute only.
A program may use at most 32 MiB of HBM per device.

```python
import math
import jax
import jax.numpy as jnp

COOL_STEPS = 8
NX = 512
NY = 256
NZ = 64


def draw_corona(key, part):
    lower_key = jax.random.fold_in(key, 11)
    upper_key = jax.random.fold_in(key, 23)
    extra_key = jax.random.fold_in(key, 37)
    lower_height = jax.random.randint(lower_key, (), NZ // 4, 3 * NZ // 8 + 1)
    upper_height = jax.random.randint(upper_key, (), NZ // 4, 3 * NZ // 8 + 1)
    index = jnp.arange(NZ, dtype=jnp.int32)
    offsets = jnp.abs(2 * index + 1 - NZ)
    threshold = jnp.where(2 * index < NZ, lower_height, upper_height)
    outer = offsets > 2 * threshold
    extra = jax.random.randint(extra_key, (NZ,), 0, 4) == 0
    return jnp.logical_or(outer, extra).astype(jnp.int32)


def shard_levels(own_key, dims, split, least, largest):
    def one(axis_at, shards_of):
        draws = jax.random.uniform(jax.random.fold_in(jax.random.fold_in(own_key, 6), axis_at), (shards_of,), jnp.float32, least / len(split), largest / len(split))
        return jnp.repeat(jnp.exp(draws), dims[axis_at] // shards_of).reshape((-1,) + (1,) * (len(dims) - axis_at - 1))

    level = one(*split[0])
    for cut in split[1:]:
        level = level * one(*cut)
    return level


def noise(stream_key, extent, scale, limit, cuts=(), kind=jnp.bfloat16):
    level = shard_levels(stream_key, extent, cuts, -0.22, 0.18) if cuts else 1.0
    values = jax.random.normal(stream_key, extent, jnp.float32) * scale * level
    return jnp.minimum(jnp.maximum(values, -limit), limit).astype(kind)


def setup_inputs(seed: int = 0) -> dict:
    splits = jax.random.split(jax.random.key(seed), 6)
    density = jnp.clip(jnp.exp(math.log(3.0) - 2.3025851 * jax.random.uniform(splits[0], (NZ, NY, NX), jnp.float32) ** shard_levels(splits[0], (NZ, NY, NX), ((0, 8), (1, 32), (2, 4)), -0.2, 0.2)), 0.3, 3.0)
    velocity = noise(splits[1], (3, NZ, NY, NX), 0.5, 3.0, ((1, 8), (2, 32), (3, 4)), jnp.float32)
    pressure = jnp.clip(jnp.exp(math.log(3.0) - 2.3025851 * jax.random.uniform(splits[2], (NZ, NY, NX), jnp.float32) ** shard_levels(splits[2], (NZ, NY, NX), ((0, 8), (1, 32), (2, 4)), -0.2, 0.2)), 0.3, 3.0)
    field = noise(splits[3], (3, NZ, NY, NX), 0.5, 3.0, ((1, 8), (2, 32), (3, 4)), jnp.float32)
    corona = draw_corona(jax.random.fold_in(splits[5], 71), 0)
    return {"density": density, "velocity": velocity, "pressure": pressure, "field": field, "corona": corona}


adiabatic = 5.0 / 3.0
courant = 0.08
cool_rate = 0.03
gravity = 1.0
cyclic_pairs = ((2, 1), (0, 2), (1, 0))

def shift_up(values, along):
    return jnp.roll(values, -1, along)

def shift_down(values, along):
    return jnp.roll(values, 1, along)

def cool_cells(density, pressure):
    for subcycle in range(COOL_STEPS):
        pressure = pressure / (1.0 + cool_rate * jnp.sqrt(density * pressure))
    return pressure

def state_terms(density, velocity, pressure, magnetic, normal_axis):
    others = [component for component in range(3) if component != normal_axis]
    normal_field = magnetic[normal_axis]
    transverse = magnetic[others[0]] * magnetic[others[0]] + magnetic[others[1]] * magnetic[others[1]]
    squared = transverse + normal_field * normal_field
    total_pressure = pressure + 0.5 * squared
    kinetic = velocity[0] * velocity[0] + velocity[1] * velocity[1] + velocity[2] * velocity[2]
    alignment = velocity[0] * magnetic[0] + velocity[1] * magnetic[1] + velocity[2] * magnetic[2]
    energy = pressure / (adiabatic - 1.0) + 0.5 * density * kinetic + 0.5 * squared
    sound = adiabatic * pressure / density
    along_field = normal_field * normal_field / density
    across_field = transverse / density
    fast_speed = jnp.sqrt(0.5 * (sound + along_field + across_field + jnp.sqrt((sound - along_field - across_field) ** 2 + 4.0 * sound * across_field)))
    normal_speed = velocity[normal_axis]
    conserved = [density] + [density * velocity[component] for component in range(3)] + [energy] + [magnetic[component] for component in others]
    fluxes = [density * normal_speed]
    for component in range(3):
        moment = density * velocity[component] * normal_speed - magnetic[component] * normal_field
        if component == normal_axis:
            moment = moment + total_pressure
        fluxes.append(moment)
    fluxes.append((energy + total_pressure) * normal_speed - normal_field * alignment)
    for component in others:
        fluxes.append(normal_speed * magnetic[component] - velocity[component] * normal_field)
    return (normal_speed, fast_speed, conserved, fluxes)

def interface_flux(density, velocity, pressure, centre, normal_face, normal_axis):
    lower_field = [shift_down(member, normal_axis) for member in centre]
    lower_field[normal_axis] = normal_face
    upper_field = list(centre)
    upper_field[normal_axis] = normal_face
    lower_terms = state_terms(shift_down(density, normal_axis), [shift_down(member, normal_axis) for member in velocity], shift_down(pressure, normal_axis), lower_field, normal_axis)
    upper_terms = state_terms(density, velocity, pressure, upper_field, normal_axis)
    slowest = jnp.minimum(jnp.minimum(lower_terms[0] - lower_terms[1], upper_terms[0] - upper_terms[1]), 0.0)
    fastest = jnp.maximum(jnp.maximum(lower_terms[0] + lower_terms[1], upper_terms[0] + upper_terms[1]), 0.0)
    inverse = 1.0 / (fastest - slowest)
    result = []
    for member in range(7):
        lower_flux = lower_terms[3][member]
        upper_flux = upper_terms[3][member]
        jump = upper_terms[2][member] - lower_terms[2][member]
        result.append((fastest * lower_flux - slowest * upper_flux + slowest * fastest * jump) * inverse)
    return result

def advance(extended, height):
    density = extended[0]
    velocity = [extended[1], extended[2], extended[3]]
    pressure = extended[4]
    faces = [extended[5], extended[6], extended[7]]
    centre = [0.5 * (faces[component] + shift_up(faces[component], component)) for component in range(3)]
    fluxes = [interface_flux(density, velocity, pressure, centre, faces[direction], direction) for direction in range(3)]
    kinetic = velocity[0] * velocity[0] + velocity[1] * velocity[1] + velocity[2] * velocity[2]
    squared = centre[0] * centre[0] + centre[1] * centre[1] + centre[2] * centre[2]
    energy = pressure / (adiabatic - 1.0) + 0.5 * density * kinetic + 0.5 * squared
    conserved = [density, density * velocity[0], density * velocity[1], density * velocity[2], energy]
    inner = (slice(2, -2), slice(2, -2), slice(2, -2))
    updated = []
    for member in range(5):
        change = jnp.zeros_like(density)
        for direction in range(3):
            change = change + shift_up(fluxes[direction][member], direction) - fluxes[direction][member]
        updated.append((conserved[member] - courant * change)[inner])
    pull = -gravity * height[:, None, None]
    updated[1] = updated[1] + courant * density[inner] * pull
    updated[4] = updated[4] + courant * density[inner] * velocity[0][inner] * pull
    electric = []
    for edge in range(3):
        first, second = cyclic_pairs[edge]
        first_others = [component for component in range(3) if component != first]
        second_others = [component for component in range(3) if component != second]
        first_flux = fluxes[first][5 + first_others.index(second)]
        second_flux = fluxes[second][5 + second_others.index(first)]
        electric.append(0.25 * (second_flux + shift_down(second_flux, first) - first_flux - shift_down(first_flux, second)))
    new_faces = []
    for component in range(3):
        across, beyond = cyclic_pairs[component]
        curl = shift_up(electric[beyond], across) - electric[beyond] - (shift_up(electric[across], beyond) - electric[across])
        new_faces.append((faces[component] - courant * curl)[inner])
    return (jnp.stack(updated), jnp.stack(new_faces))

def reference(density, velocity, pressure, field, corona):
    cooled = jnp.where(corona[:, None, None] == 1, cool_cells(density, pressure), pressure)
    stacked = jnp.concatenate([density[None], velocity, cooled[None], field], 0)
    extended = jnp.pad(stacked, ((0, 0), (0, 0), (0, 0), (2, 2)), mode='wrap')
    extended = jnp.pad(extended, ((0, 0), (0, 0), (2, 2), (0, 0)), mode='edge')
    extended = jnp.pad(extended, ((0, 0), (2, 2), (0, 0), (0, 0)), mode='edge')
    height = (2 * jnp.arange(NZ, dtype=jnp.int32) + 1 - NZ).astype(jnp.float32) / NZ
    return advance(extended, height)
```

```python
import jax
import jax.numpy as jnp
from jax import lax
from jax.experimental import pallas as pl
from jax.experimental.pallas import tpu as pltpu
from jax.sharding import PartitionSpec as P

COOL_STEPS = 8
GAMMA = 5.0 / 3.0
COURANT = 0.08
COOL_RATE = 0.03
GRAVITY = 1.0

NZ, NY, NX = 8, 8, 128
ROWS = 10
UP_ROWS, DOWN_ROWS = 88, 96
Z_MAIN = range(NZ)

f32 = jnp.float32


def gather_block(density, velocity, pressure, field, own, top, bottom, sems):
    one = pl.ds(0, 1)
    copies = []
    for out, z in ((top, NZ - 1), (bottom, 0)):
        copies += [
            (density.at[pl.ds(z, 1)], out.at[one]),
            (velocity.at[:, z], out.at[pl.ds(1, 3)]),
            (pressure.at[pl.ds(z, 1)], out.at[pl.ds(4, 1)]),
            (field.at[:, z], out.at[pl.ds(5, 3)]),
        ]
    copies += [
        (field.at[0, pl.ds(1, 1)], bottom.at[pl.ds(8, 1)]),
        (density, own.at[0]),
        (velocity, own.at[pl.ds(1, 3)]),
        (pressure, own.at[4]),
        (field, own.at[pl.ds(5, 3)]),
    ]
    copies = [pltpu.make_async_copy(a, b, sems.at[i]) for i, (a, b) in enumerate(copies)]
    for copy in copies:
        copy.start()
    for copy in copies:
        copy.wait()


def pack_rows(own, below, above, up, down):
    lowest = lax.axis_index("gz") == 0
    highest = lax.axis_index("gz") == lax.axis_size("gz") - 1

    def put(out, at, row):
        out[pl.ds(at, 1), :] = row

    for out, y in ((up, NY - 1), (down, 0)):
        for member in range(8):
            base = member * ROWS
            for z in Z_MAIN:
                put(out, base + 1 + z, own[member, z, pl.ds(y, 1), :])
            put(out, base, below[member, pl.ds(y, 1), :])
            put(out, base + 9, above[member, pl.ds(y, 1), :])
        put(out, 80, above[8, pl.ds(y, 1), :])
    for z in Z_MAIN:
        put(down, 82 + z, own[6, z, pl.ds(1, 1), :])
    put(down, 81, below[6, pl.ds(1, 1), :])
    put(down, 90, above[6, pl.ds(1, 1), :])

    @pl.when(lowest)
    def _():
        for out, y in ((up, NY - 1), (down, 0)):
            for member in range(8):
                put(out, member * ROWS, own[member, 0, pl.ds(y, 1), :])
        put(down, 81, own[6, 0, pl.ds(1, 1), :])

    @pl.when(highest)
    def _():
        for out, y in ((up, NY - 1), (down, 0)):
            for member in range(8):
                put(out, member * ROWS + 9, own[member, NZ - 1, pl.ds(y, 1), :])
            put(out, 80, own[5, NZ - 1, pl.ds(y, 1), :])
        put(down, 90, own[6, NZ - 1, pl.ds(1, 1), :])


def lanes():
    return lax.broadcasted_iota(jnp.int32, (8, NX), 1)


def sublanes():
    return lax.broadcasted_iota(jnp.int32, (8, NX), 0)


def roll(values, by, axis):
    size = values.shape[axis]
    by = by % size
    return values if by == 0 else pltpu.roll(values, by, axis)


def cool(density, pressure):
    for _ in range(COOL_STEPS):
        pressure = pressure / (1.0 + COOL_RATE * jnp.sqrt(density * pressure))
    return pressure


def pack_columns(corona, own, below, above, left_rows, right_rows, ext, cols):
    row_at, row_count = lax.axis_index("gy"), lax.axis_size("gy")
    slab_at, slab_count = lax.axis_index("gz"), lax.axis_size("gz")
    for member in range(8):
        for z in Z_MAIN:
            ext[member, z + 1, 0:8, :] = own[member, z]
        ext[member, 0, 0:8, :] = below[member]
        ext[member, 9, 0:8, :] = above[member]
    ext[5, 10, 0:8, :] = above[8]

    @pl.when(slab_at == 0)
    def _():
        for member in range(8):
            ext[member, 0, 0:8, :] = own[member, 0]

    @pl.when(slab_at == slab_count - 1)
    def _():
        for member in range(8):
            ext[member, 9, 0:8, :] = own[member, NZ - 1]
        ext[5, 10, 0:8, :] = own[5, NZ - 1]

    where = [(member, z, member * ROWS + z) for member in range(8) for z in range(ROWS)] + [(5, 10, 80)]
    for member, z, at in where:
        ext[member, z, 15:16, :] = left_rows[pl.ds(at, 1), :]
        ext[member, z, 8:9, :] = right_rows[pl.ds(at, 1), :]
    for z in range(ROWS):
        ext[6, z, 9:10, :] = right_rows[pl.ds(81 + z, 1), :]

    @pl.when(row_at == 0)
    def _():
        for member, z, _at in where:
            ext[member, z, 15:16, :] = ext[member, z, 0:1, :]

    @pl.when(row_at == row_count - 1)
    def _():
        for member, z, _at in where:
            ext[member, z, 8:9, :] = ext[member, z, 7:8, :]
        for z in range(ROWS):
            ext[6, z, 9:10, :] = ext[6, z, 7:8, :]

    tiles = [(z, t) for z in range(ROWS) for t in range(2)]
    rho = [ext[0, z, 8 * t : 8 * t + 8, :] for z, t in tiles]
    raw = [ext[4, z, 8 * t : 8 * t + 8, :] for z, t in tiles]
    now = list(raw)
    for _ in range(COOL_STEPS):
        now = [p / (1.0 + COOL_RATE * jnp.sqrt(r * p)) for r, p in zip(rho, now)]
    last = slab_count * NZ - 1
    for (z, t), p, q in zip(tiles, raw, now):
        mark = corona[jnp.clip(slab_at * NZ + z - 1, 0, last)]
        ext[4, z, 8 * t : 8 * t + 8, :] = jnp.where(jnp.full((8, NX), mark, jnp.int32) == 1, q, p)

    lane = lanes()
    for t in range(2):
        rows = slice(8 * t, 8 * t + 8)
        low = jnp.zeros((8, NX), f32)
        high = jnp.zeros((8, NX), f32)
        second = jnp.zeros((8, NX), f32)
        for z in range(11):
            for member in range(8) if z < 10 else (5,):
                at = 8 * z + member
                tile = ext[member, z, rows, :]
                low = jnp.where(lane == at, roll(tile, at, 1), low)
                high = jnp.where(lane == at, roll(tile, at + 1, 1), high)
                if member == 7:
                    second = jnp.where(lane == 8 * z + 2, roll(tile, 8 * z + 1, 1), second)
        cols[0, rows, :] = low
        cols[1, rows, :] = high
        cols[2, rows, :] = second


class Cell:
    def __init__(self, rho, vel, p, cen):
        self.rho, self.vel, self.p, self.cen = rho, vel, p, cen
        self.mom = [rho * v for v in vel]
        kinetic = self.mom[0] * vel[0] + self.mom[1] * vel[1] + self.mom[2] * vel[2]
        self.thermal = p * (1.0 / (GAMMA - 1.0)) + 0.5 * kinetic
        self.inv = 1.0 / rho
        self.sound = GAMMA * p * self.inv


def state(cell, normal, axis):
    b, c = [k for k in range(3) if k != axis]
    vel, cen = cell.vel, cell.cen
    across = cen[b] * cen[b] + cen[c] * cen[c]
    square = normal * normal
    half = 0.5 * (across + square)
    total = cell.p + half
    energy = cell.thermal + half
    n, t, s = square * cell.inv, across * cell.inv, cell.sound
    gap = s - n - t
    fast = jnp.sqrt(0.5 * (s + n + t + jnp.sqrt(gap * gap + 4.0 * s * t)))
    align = vel[axis] * normal + vel[b] * cen[b] + vel[c] * cen[c]
    va = vel[axis]
    flux = [cell.mom[axis]]
    for k in range(3):
        if k == axis:
            flux.append(cell.mom[k] * va - square + total)
        else:
            flux.append(cell.mom[k] * va - cen[k] * normal)
    flux.append((energy + total) * va - normal * align)
    for k in (b, c):
        flux.append(va * cen[k] - vel[k] * normal)
    held = [cell.rho] + cell.mom + [energy, cen[b], cen[c]]
    return va, fast, held, flux


def hll(lower, upper, normal, axis, members):
    lv, lf, lu, lflux = state(lower, normal, axis)
    uv, uf, uu, uflux = state(upper, normal, axis)
    slow = jnp.minimum(jnp.minimum(lv - lf, uv - uf), 0.0)
    fast = jnp.maximum(jnp.maximum(lv + lf, uv + uf), 0.0)
    inverse = 1.0 / (fast - slow)
    a, b = fast * inverse, slow * inverse
    c = slow * a
    return {m: a * lflux[m] - b * uflux[m] + c * (uu[m] - lu[m]) for m in members}


def member_of(axis, component):
    return 5 + [k for k in range(3) if k != axis].index(component)


def advance(gathered, own_cols, ext, conserved, faces_new):
    lane, sub = lanes(), sublanes()
    size = lax.axis_size("gx")
    at = lax.axis_index("gx")
    left, right = lax.rem(at + size - 1, size), lax.rem(at + 1, size)
    first_lane, last_lane = lane == 0, lane == NX - 1
    first_row, last_row = sub == 0, sub == 7
    slot = lane % 8

    def down_y(q):
        r0, r1 = roll(q[0], 1, 0), roll(q[1], 1, 0)
        return [jnp.where(first_row, r1, r0), jnp.where(first_row, r0, r1)]

    def up_y(q):
        r0, r1 = roll(q[0], -1, 0), roll(q[1], -1, 0)
        return [jnp.where(last_row, r1, r0), jnp.where(last_row, r0, r1)]

    def down_x(q, side, source):
        return jnp.where(first_lane, roll(side, -source, 1), roll(q, 1, 1))

    def up_x(q, side, source):
        return jnp.where(last_lane, roll(side, NX - 1 - source, 1), roll(q, -1, 1))

    low_r = [gathered[right, 0, 8 * t : 8 * t + 8, :] for t in range(2)]
    two_r = [gathered[right, 2, 8 * t : 8 * t + 8, :] for t in range(2)]
    high_l = [gathered[left, 1, 8 * t : 8 * t + 8, :] for t in range(2)]
    own_low = [own_cols[0, 8 * t : 8 * t + 8, :] for t in range(2)]
    own_high = [own_cols[1, 8 * t : 8 * t + 8, :] for t in range(2)]

    def column(member):
        out = []
        for t in range(2):
            v = roll(own_high[t], -member, 1)
            v = jnp.where(slot == 1, roll(low_r[t], 1 - member, 1), v)
            v = jnp.where(slot == 3, roll(high_l[t], 3 - member, 1), v)
            v = jnp.where(slot == 4, roll(own_low[t], 4 - member, 1), v)
            if member == 7:
                v = jnp.where(slot == 2, two_r[t], v)
            out.append(v)
        return out

    col = [column(member) for member in range(8)]
    col_next_y = up_y(col[6])
    col_cen = [
        [0.5 * (v + roll(v, -8, 1)) for v in col[5]],
        [0.5 * (v + n) for v, n in zip(col[6], col_next_y)],
        [0.5 * (v + roll(v, -1, 1)) for v in col[7]],
    ]

    def cells(prim, cen):
        return [Cell(prim[0][t], [prim[k][t] for k in (1, 2, 3)], prim[4][t], [cen[k][t] for k in range(3)]) for t in range(2)]

    col_cell = cells(col, col_cen)
    shifted = lambda by: cells(
        [[roll(v, by, 1) for v in col[k]] for k in range(5)],
        [[roll(v, by, 1) for v in col_cen[k]] for k in range(3)],
    )
    full = tuple(range(7))
    col_x_lower, col_z_lower = shifted(1), shifted(8)
    col_y_lower = cells([down_y(col[k]) for k in range(5)], [down_y(col_cen[k]) for k in range(3)])
    XB = {(a, k): member_of(a, k) for a in range(3) for k in range(3) if a != k}
    col_fx = [hll(col_x_lower[0], col_cell[0], col[7][0], 2, full), hll(col_x_lower[1], col_cell[1], col[7][1], 2, (XB[2, 1],))]
    col_fy = [hll(col_y_lower[t], col_cell[t], col[6][t], 1, (XB[1, 2],))[XB[1, 2]] for t in range(2)]
    col_fz = hll(col_z_lower[0], col_cell[0], col[5][0], 0, (XB[0, 2],))[XB[0, 2]]
    fx_by = [f[XB[2, 1]] for f in col_fx]
    fx_bz = col_fx[0][XB[2, 0]]
    down = down_y(fx_by)
    col_ez = [0.25 * (col_fy[t] + roll(col_fy[t], 1, 1) - fx_by[t] - down[t]) for t in range(2)]
    col_ey = 0.25 * (fx_bz + roll(fx_bz, 8, 1) - col_fz - roll(col_fz, 1, 1))

    def slab_cells(z):
        base = 8 * (z + 1)
        get = lambda member, s: [ext[member, s, 0:8, :], ext[member, s, 8:16, :]]
        prim = [get(member, z + 1) for member in range(8)]
        next_z = get(5, z + 2)
        next_y = up_y(prim[6])
        next_x = [up_x(prim[7][t], low_r[t], base + 7) for t in range(2)]
        cen = [
            [0.5 * (prim[5][t] + next_z[t]) for t in range(2)],
            [0.5 * (prim[6][t] + next_y[t]) for t in range(2)],
            [0.5 * (prim[7][t] + next_x[t]) for t in range(2)],
        ]
        return prim, cen, cells(prim, cen)

    def slab_fluxes(z, prim, cen, here, below):
        base = 8 * (z + 1)
        inside = 0 <= z < NZ
        fz = fy = fx = None
        if z >= 0:
            fz = [
                hll(below[0], here[0], prim[5][0], 0, full),
                hll(below[1], here[1], prim[5][1], 0, (XB[0, 1],)),
            ]
        y_lower = cells([down_y(prim[k]) for k in range(5)], [down_y(cen[k]) for k in range(3)])
        x_lower = []
        for t in range(2):
            p = [down_x(prim[k][t], high_l[t], base + k) for k in range(5)]
            c = [down_x(cen[k][t], col_cen[k][t], base + 3) for k in range(3)]
            x_lower.append(Cell(p[0], p[1:4], p[4], c))
        members = full if inside else (XB[1, 0],)
        fy = [hll(y_lower[t], here[t], prim[6][t], 1, members) for t in range(2)]
        if inside:
            fx = [
                hll(x_lower[0], here[0], prim[7][0], 2, full),
                hll(x_lower[1], here[1], prim[7][1], 2, (XB[2, 1],)),
            ]
        else:
            fx = [hll(x_lower[0], here[0], prim[7][0], 2, (XB[2, 0],)), None]
        return fz, fy, fx

    slabs = lax.axis_size("gz") * NZ
    first_slab = lax.axis_index("gz") * NZ
    previous = None
    for z in range(-1, NZ + 1):
        base = 8 * (z + 1)
        prim, cen, here = slab_cells(z)
        below = previous["here"] if previous else None
        fz, fy, fx = slab_fluxes(z, prim, cen, here, below)
        now = dict(prim=prim, cen=cen, here=here, fz=fz, fy=fy, fx=fx, base=base)
        if z >= 0:
            by = [fz[t][XB[0, 1]] for t in range(2)]
            by_down = down_y(by)
            now["ex"] = [0.25 * (by[t] + by_down[t] - fy[t][XB[1, 0]] - previous["fy"][t][XB[1, 0]]) for t in range(2)]
            bx = fz[0][XB[0, 2]]
            now["ey"] = 0.25 * (fx[0][XB[2, 0]] + previous["fx"][0][XB[2, 0]] - bx - down_x(bx, col_fz, base + 3))
        if 0 <= z < NZ:
            bx = [fy[t][XB[1, 2]] for t in range(2)]
            by = [fx[t][XB[2, 1]] for t in range(2)]
            by_down = down_y(by)
            now["ez"] = [0.25 * (bx[t] + down_x(bx[t], col_fy[t], base + 3) - by[t] - by_down[t]) for t in range(2)]
        if z >= 1:
            k = z - 1
            was = previous
            cell = was["here"][0]
            pull = -GRAVITY * (2 * (first_slab + k) + 1 - slabs).astype(f32) / slabs
            squared = sum(c[0] * c[0] for c in was["cen"])
            held = [cell.rho] + cell.mom + [cell.thermal + 0.5 * squared]
            for m in range(5):
                y_next = up_y([was["fy"][t][m] for t in range(2)])[0]
                x_next = up_x(was["fx"][0][m], col_fx[0][m], was["base"] + 1)
                change = (fz[0][m] - was["fz"][0][m]) + (y_next - was["fy"][0][m]) + (x_next - was["fx"][0][m])
                value = held[m] - COURANT * change
                if m == 1:
                    value = value + (COURANT * pull) * cell.rho
                if m == 4:
                    value = value + (COURANT * pull) * cell.mom[0]
                conserved[m, k] = value
            ex, ey, ez = was["ex"], was["ey"], was["ez"]
            ex_up_y, ez_up_y = up_y(ex)[0], up_y(ez)[0]
            ey_up_x = up_x(ey, col_ey, was["base"] + 1)
            ez_up_x = up_x(ez[0], col_ez[0], was["base"] + 1)
            curls = (
                ey_up_x - ey - (ex_up_y - ex[0]),
                now["ex"][0] - ex[0] - (ez_up_x - ez[0]),
                ez_up_y - ez[0] - (now["ey"] - ey),
            )
            for c in range(3):
                faces_new[c, k] = was["prim"][5 + c][0] - COURANT * curls[c]
        previous = now


VMEM = pl.BlockSpec(memory_space=pltpu.VMEM)
SMEM = pl.BlockSpec(memory_space=pltpu.SMEM)


def shape(*dims):
    return jax.ShapeDtypeStruct(dims, f32)


def held(*dims):
    return pltpu.VMEM(dims, f32)


def near(*arrays):
    return [pltpu.with_memory_space_constraint(a, pltpu.VMEM) for a in arrays]


def neighbours(axis):
    count = lax.axis_size(axis)
    return [(i, i + 1) for i in range(count - 1)], [(i + 1, i) for i in range(count - 1)]


def on_device(density, velocity, pressure, field, corona):
    own, top, bottom = pl.pallas_call(
        gather_block,
        out_shape=(held(8, NZ, NY, NX), held(8, NY, NX), held(9, NY, NX)),
        in_specs=[pl.BlockSpec(memory_space=pl.ANY)] * 4,
        out_specs=(VMEM,) * 3,
        scratch_shapes=[pltpu.SemaphoreType.DMA((13,))],
        name="gather_block",
    )(density, velocity, pressure, field)
    up, down = neighbours("gz")
    below = lax.ppermute(top, "gz", up)
    above = lax.ppermute(bottom, "gz", down)
    rows_up, rows_down = pl.pallas_call(
        pack_rows,
        out_shape=(held(UP_ROWS, NX), held(DOWN_ROWS, NX)),
        in_specs=[VMEM] * 3,
        out_specs=(VMEM, VMEM),
        name="pack_rows",
    )(*near(own, below, above))
    up, down = neighbours("gy")
    left_rows = lax.ppermute(rows_up, "gy", up)
    right_rows = lax.ppermute(rows_down, "gy", down)
    ext, cols = pl.pallas_call(
        pack_columns,
        out_shape=(held(8, 11, 16, NX), held(3, 16, NX)),
        in_specs=[SMEM] + [VMEM] * 5,
        out_specs=(VMEM, VMEM),
        name="pack_columns",
    )(corona, *near(own, below, above, left_rows, right_rows))
    gathered = lax.all_gather(cols, "gx", axis=0)
    return pl.pallas_call(
        advance,
        out_shape=(shape(5, NZ, NY, NX), shape(3, NZ, NY, NX)),
        in_specs=[VMEM] * 3,
        out_specs=(VMEM, VMEM),
        name="advance",
    )(*near(gathered, cols, ext))


def solution(mesh):
    block = P("gz", "gy", "gx")
    blocks = P(None, "gz", "gy", "gx")
    return jax.shard_map(
        on_device,
        mesh=mesh,
        in_specs=(block, blocks, block, blocks, P()),
        out_specs=(blocks, blocks),
        check_vma=False,
    )
```

```python
import jax
import jax.numpy as jnp
from jax import lax
from jax.experimental import pallas as pl
from jax.experimental.pallas import tpu as pltpu
from jax.sharding import PartitionSpec as P


COOL_STEPS = 8
GAMMA = 5.0 / 3.0
COURANT = 0.08
COOL_RATE = 0.03
GRAVITY = 1.0

NZ, NY, NX = 8, 8, 128
ROWS = 10
UP_ROWS, DOWN_ROWS = 88, 96
Z_MAIN = range(NZ)

f32 = jnp.float32


def gather_block(density, velocity, pressure, field, own, top, bottom, sems):
    one = pl.ds(0, 1)
    copies = []
    for out, z in ((top, NZ - 1), (bottom, 0)):
        copies += [
            (density.at[pl.ds(z, 1)], out.at[one]),
            (velocity.at[:, z], out.at[pl.ds(1, 3)]),
            (pressure.at[pl.ds(z, 1)], out.at[pl.ds(4, 1)]),
            (field.at[:, z], out.at[pl.ds(5, 3)]),
        ]
    copies += [
        (field.at[0, pl.ds(1, 1)], bottom.at[pl.ds(8, 1)]),
        (density, own.at[0]),
        (velocity, own.at[pl.ds(1, 3)]),
        (pressure, own.at[4]),
        (field, own.at[pl.ds(5, 3)]),
    ]
    copies = [pltpu.make_async_copy(a, b, sems.at[i]) for i, (a, b) in enumerate(copies)]
    for copy in copies:
        copy.start()
    for copy in copies:
        copy.wait()


def pack_rows(own, below, above, up, down):
    lowest = lax.axis_index("gz") == 0
    highest = lax.axis_index("gz") == lax.axis_size("gz") - 1

    def put(out, at, row):
        out[pl.ds(at, 1), :] = row

    for out, y in ((up, NY - 1), (down, 0)):
        for member in range(8):
            base = member * ROWS
            for z in Z_MAIN:
                put(out, base + 1 + z, own[member, z, pl.ds(y, 1), :])
            put(out, base, below[member, pl.ds(y, 1), :])
            put(out, base + 9, above[member, pl.ds(y, 1), :])
        put(out, 80, above[8, pl.ds(y, 1), :])
    for z in Z_MAIN:
        put(down, 82 + z, own[6, z, pl.ds(1, 1), :])
    put(down, 81, below[6, pl.ds(1, 1), :])
    put(down, 90, above[6, pl.ds(1, 1), :])

    @pl.when(lowest)
    def _():
        for out, y in ((up, NY - 1), (down, 0)):
            for member in range(8):
                put(out, member * ROWS, own[member, 0, pl.ds(y, 1), :])
        put(down, 81, own[6, 0, pl.ds(1, 1), :])

    @pl.when(highest)
    def _():
        for out, y in ((up, NY - 1), (down, 0)):
            for member in range(8):
                put(out, member * ROWS + 9, own[member, NZ - 1, pl.ds(y, 1), :])
            put(out, 80, own[5, NZ - 1, pl.ds(y, 1), :])
        put(down, 90, own[6, NZ - 1, pl.ds(1, 1), :])


def lanes():
    return lax.broadcasted_iota(jnp.int32, (8, NX), 1)


def sublanes():
    return lax.broadcasted_iota(jnp.int32, (8, NX), 0)


def roll(values, by, axis):
    size = values.shape[axis]
    by = by % size
    return values if by == 0 else pltpu.roll(values, by, axis)


def marks_of(corona):
    first, last = lax.axis_index("gz") * NZ, lax.axis_size("gz") * NZ - 1
    return [corona[jnp.clip(first + z - 1, 0, last)] for z in range(ROWS)]


def cool(corona, ext):
    rho = [ext[0, z] for z in range(ROWS)]
    raw = [ext[4, z] for z in range(ROWS)]
    now = list(raw)
    for _ in range(COOL_STEPS):
        now = [p / (1.0 + COOL_RATE * jnp.sqrt(r * p)) for r, p in zip(rho, now)]
    for z, (mark, p, q) in enumerate(zip(marks_of(corona), raw, now)):
        ext[4, z] = jnp.where(jnp.full((8, NX), mark, jnp.int32) == 1, q, p)


def columns_of(ext):
    lane = lanes()
    low = high = second = jnp.zeros((8, NX), f32)
    for z in range(11):
        for member in range(8) if z < 10 else (5,):
            at = 8 * z + member
            tile = ext[member, z]
            low = jnp.where(lane == at, roll(tile, at, 1), low)
            high = jnp.where(lane == at, roll(tile, at + 1, 1), high)
            if member == 7:
                second = jnp.where(lane == 8 * z + 2, roll(tile, 8 * z + 1, 1), second)
    return low, high, second


def pack_main(corona, own, below, above, ext, cols):
    slab_at, slab_count = lax.axis_index("gz"), lax.axis_size("gz")
    for member in range(8):
        for z in Z_MAIN:
            ext[member, z + 1] = own[member, z]
        ext[member, 0] = below[member]
        ext[member, 9] = above[member]
    ext[5, 10] = above[8]

    @pl.when(slab_at == 0)
    def _():
        for member in range(8):
            ext[member, 0] = own[member, 0]

    @pl.when(slab_at == slab_count - 1)
    def _():
        for member in range(8):
            ext[member, 9] = own[member, NZ - 1]
        ext[5, 10] = own[5, NZ - 1]

    cool(corona, ext)
    for i, v in enumerate(columns_of(ext)):
        cols[i] = v


PLACES = [(member, z, member * ROWS + z) for member in range(8) for z in range(ROWS)] + [(5, 10, 80)]


def pack_edges(corona, main, main_cols, left_rows, right_rows, ext, cols):
    row_at, row_count = lax.axis_index("gy"), lax.axis_size("gy")
    for member, z, at in PLACES:
        ext[member, z, 7:8, :] = left_rows[pl.ds(at, 1), :]
        ext[member, z, 0:1, :] = right_rows[pl.ds(at, 1), :]
    for z in range(ROWS):
        ext[6, z, 1:2, :] = right_rows[pl.ds(81 + z, 1), :]
    cool(corona, ext)

    @pl.when(row_at == 0)
    def _():
        for member, z, _at in PLACES:
            ext[member, z, 7:8, :] = main[member, z, 0:1, :]

    @pl.when(row_at == row_count - 1)
    def _():
        for member, z, _at in PLACES:
            ext[member, z, 0:1, :] = main[member, z, 7:8, :]
        for z in range(ROWS):
            ext[6, z, 1:2, :] = main[6, z, 7:8, :]

    for i, v in enumerate(columns_of(ext)):
        cols[i, 0:8, :] = main_cols[i]
        cols[i, 8:16, :] = v


class Cell:
    def __init__(self, rho, vel, p, cen):
        self.rho, self.vel, self.p, self.cen = rho, vel, p, cen
        self.mom = [rho * v for v in vel]
        kinetic = self.mom[0] * vel[0] + self.mom[1] * vel[1] + self.mom[2] * vel[2]
        self.thermal = p * (1.0 / (GAMMA - 1.0)) + 0.5 * kinetic
        self.inv = 1.0 / rho
        self.sound = GAMMA * p * self.inv


def state(cell, normal, axis):
    b, c = [k for k in range(3) if k != axis]
    vel, cen = cell.vel, cell.cen
    across = cen[b] * cen[b] + cen[c] * cen[c]
    square = normal * normal
    half = 0.5 * (across + square)
    total = cell.p + half
    energy = cell.thermal + half
    n, t, s = square * cell.inv, across * cell.inv, cell.sound
    gap = s - n - t
    fast = jnp.sqrt(0.5 * (s + n + t + jnp.sqrt(gap * gap + 4.0 * s * t)))
    align = vel[axis] * normal + vel[b] * cen[b] + vel[c] * cen[c]
    va = vel[axis]
    flux = [cell.mom[axis]]
    for k in range(3):
        if k == axis:
            flux.append(cell.mom[k] * va - square + total)
        else:
            flux.append(cell.mom[k] * va - cen[k] * normal)
    flux.append((energy + total) * va - normal * align)
    for k in (b, c):
        flux.append(va * cen[k] - vel[k] * normal)
    held = [cell.rho] + cell.mom + [energy, cen[b], cen[c]]
    return va, fast, held, flux


def hll(lower, upper, normal, axis, members):
    lv, lf, lu, lflux = state(lower, normal, axis)
    uv, uf, uu, uflux = state(upper, normal, axis)
    slow = jnp.minimum(jnp.minimum(lv - lf, uv - uf), 0.0)
    fast = jnp.maximum(jnp.maximum(lv + lf, uv + uf), 0.0)
    inverse = 1.0 / (fast - slow)
    a, b = fast * inverse, slow * inverse
    c = slow * a
    return {m: a * lflux[m] - b * uflux[m] + c * (uu[m] - lu[m]) for m in members}


def member_of(axis, component):
    return 5 + [k for k in range(3) if k != axis].index(component)


def advance(gathered, own_cols, main, edges, conserved_out, faces_out, conserved, faces_new, sems):
    lane, sub = lanes(), sublanes()
    size = lax.axis_size("gx")
    at = lax.axis_index("gx")
    left, right = lax.rem(at + size - 1, size), lax.rem(at + 1, size)
    first_lane, last_lane = lane == 0, lane == NX - 1
    first_row, last_row = sub == 0, sub == 7
    slot = lane % 8

    def down_y(q):
        r0, r1 = roll(q[0], 1, 0), roll(q[1], 1, 0)
        return [jnp.where(first_row, r1, r0), jnp.where(first_row, r0, r1)]

    def up_y(q):
        r0, r1 = roll(q[0], -1, 0), roll(q[1], -1, 0)
        return [jnp.where(last_row, r1, r0), jnp.where(last_row, r0, r1)]

    def down_x(q, side, source):
        return jnp.where(first_lane, roll(side, -source, 1), roll(q, 1, 1))

    def up_x(q, side, source):
        return jnp.where(last_lane, roll(side, NX - 1 - source, 1), roll(q, -1, 1))

    low_r = [gathered[right, 0, 8 * t : 8 * t + 8, :] for t in range(2)]
    two_r = [gathered[right, 2, 8 * t : 8 * t + 8, :] for t in range(2)]
    high_l = [gathered[left, 1, 8 * t : 8 * t + 8, :] for t in range(2)]
    own_low = [own_cols[0, 8 * t : 8 * t + 8, :] for t in range(2)]
    own_high = [own_cols[1, 8 * t : 8 * t + 8, :] for t in range(2)]

    def column(member):
        out = []
        for t in range(2):
            v = roll(own_high[t], -member, 1)
            v = jnp.where(slot == 1, roll(low_r[t], 1 - member, 1), v)
            v = jnp.where(slot == 3, roll(high_l[t], 3 - member, 1), v)
            v = jnp.where(slot == 4, roll(own_low[t], 4 - member, 1), v)
            if member == 7:
                v = jnp.where(slot == 2, two_r[t], v)
            out.append(v)
        return out

    col = [column(member) for member in range(8)]
    col_next_y = up_y(col[6])
    col_cen = [
        [0.5 * (v + roll(v, -8, 1)) for v in col[5]],
        [0.5 * (v + n) for v, n in zip(col[6], col_next_y)],
        [0.5 * (v + roll(v, -1, 1)) for v in col[7]],
    ]

    def cells(prim, cen):
        return [Cell(prim[0][t], [prim[k][t] for k in (1, 2, 3)], prim[4][t], [cen[k][t] for k in range(3)]) for t in range(2)]

    col_cell = cells(col, col_cen)
    shifted = lambda by: cells(
        [[roll(v, by, 1) for v in col[k]] for k in range(5)],
        [[roll(v, by, 1) for v in col_cen[k]] for k in range(3)],
    )
    full = tuple(range(7))
    col_x_lower, col_z_lower = shifted(1), shifted(8)
    col_y_lower = cells([down_y(col[k]) for k in range(5)], [down_y(col_cen[k]) for k in range(3)])
    XB = {(a, k): member_of(a, k) for a in range(3) for k in range(3) if a != k}
    col_fx = [hll(col_x_lower[0], col_cell[0], col[7][0], 2, full), hll(col_x_lower[1], col_cell[1], col[7][1], 2, (XB[2, 1],))]
    col_fy = [hll(col_y_lower[t], col_cell[t], col[6][t], 1, (XB[1, 2],))[XB[1, 2]] for t in range(2)]
    col_fz = hll(col_z_lower[0], col_cell[0], col[5][0], 0, (XB[0, 2],))[XB[0, 2]]
    fx_by = [f[XB[2, 1]] for f in col_fx]
    fx_bz = col_fx[0][XB[2, 0]]
    down = down_y(fx_by)
    col_ez = [0.25 * (col_fy[t] + roll(col_fy[t], 1, 1) - fx_by[t] - down[t]) for t in range(2)]
    col_ey = 0.25 * (fx_bz + roll(fx_bz, 8, 1) - col_fz - roll(col_fz, 1, 1))

    def slab_cells(z):
        base = 8 * (z + 1)
        get = lambda member, s: [main[member, s], edges[member, s]]
        prim = [get(member, z + 1) for member in range(8)]
        next_z = get(5, z + 2)
        next_y = up_y(prim[6])
        next_x = [up_x(prim[7][t], low_r[t], base + 7) for t in range(2)]
        cen = [
            [0.5 * (prim[5][t] + next_z[t]) for t in range(2)],
            [0.5 * (prim[6][t] + next_y[t]) for t in range(2)],
            [0.5 * (prim[7][t] + next_x[t]) for t in range(2)],
        ]
        return prim, cen, cells(prim, cen)

    def slab_fluxes(z, prim, cen, here, below):
        base = 8 * (z + 1)
        inside = 0 <= z < NZ
        fz = fy = fx = None
        if z >= 0:
            fz = [
                hll(below[0], here[0], prim[5][0], 0, full),
                hll(below[1], here[1], prim[5][1], 0, (XB[0, 1],)),
            ]
        y_lower = cells([down_y(prim[k]) for k in range(5)], [down_y(cen[k]) for k in range(3)])
        x_lower = []
        for t in range(2):
            p = [down_x(prim[k][t], high_l[t], base + k) for k in range(5)]
            c = [down_x(cen[k][t], col_cen[k][t], base + 3) for k in range(3)]
            x_lower.append(Cell(p[0], p[1:4], p[4], c))
        members = full if inside else (XB[1, 0],)
        fy = [hll(y_lower[t], here[t], prim[6][t], 1, members) for t in range(2)]
        if inside:
            fx = [
                hll(x_lower[0], here[0], prim[7][0], 2, full),
                hll(x_lower[1], here[1], prim[7][1], 2, (XB[2, 1],)),
            ]
        else:
            fx = [hll(x_lower[0], here[0], prim[7][0], 2, (XB[2, 0],)), None]
        return fz, fy, fx

    slabs = lax.axis_size("gz") * NZ
    first_slab = lax.axis_index("gz") * NZ
    previous = None
    copies = []
    for z in range(-1, NZ + 1):
        base = 8 * (z + 1)
        prim, cen, here = slab_cells(z)
        below = previous["here"] if previous else None
        fz, fy, fx = slab_fluxes(z, prim, cen, here, below)
        now = dict(prim=prim, cen=cen, here=here, fz=fz, fy=fy, fx=fx, base=base)
        if z >= 0:
            by = [fz[t][XB[0, 1]] for t in range(2)]
            by_down = down_y(by)
            now["ex"] = [0.25 * (by[t] + by_down[t] - fy[t][XB[1, 0]] - previous["fy"][t][XB[1, 0]]) for t in range(2)]
            bx = fz[0][XB[0, 2]]
            now["ey"] = 0.25 * (fx[0][XB[2, 0]] + previous["fx"][0][XB[2, 0]] - bx - down_x(bx, col_fz, base + 3))
        if 0 <= z < NZ:
            bx = [fy[t][XB[1, 2]] for t in range(2)]
            by = [fx[t][XB[2, 1]] for t in range(2)]
            by_down = down_y(by)
            now["ez"] = [0.25 * (bx[t] + down_x(bx[t], col_fy[t], base + 3) - by[t] - by_down[t]) for t in range(2)]
        if z >= 1:
            k = z - 1
            was = previous
            cell = was["here"][0]
            pull = -GRAVITY * (2 * (first_slab + k) + 1 - slabs).astype(f32) / slabs
            squared = sum(c[0] * c[0] for c in was["cen"])
            held = [cell.rho] + cell.mom + [cell.thermal + 0.5 * squared]
            for m in range(5):
                y_next = up_y([was["fy"][t][m] for t in range(2)])[0]
                x_next = up_x(was["fx"][0][m], col_fx[0][m], was["base"] + 1)
                change = (fz[0][m] - was["fz"][0][m]) + (y_next - was["fy"][0][m]) + (x_next - was["fx"][0][m])
                value = held[m] - COURANT * change
                if m == 1:
                    value = value + (COURANT * pull) * cell.rho
                if m == 4:
                    value = value + (COURANT * pull) * cell.mom[0]
                conserved[m, k] = value
            ex, ey, ez = was["ex"], was["ey"], was["ez"]
            ex_up_y, ez_up_y = up_y(ex)[0], up_y(ez)[0]
            ey_up_x = up_x(ey, col_ey, was["base"] + 1)
            ez_up_x = up_x(ez[0], col_ez[0], was["base"] + 1)
            curls = (
                ey_up_x - ey - (ex_up_y - ex[0]),
                now["ex"][0] - ex[0] - (ez_up_x - ez[0]),
                ez_up_y - ez[0] - (now["ey"] - ey),
            )
            for c in range(3):
                faces_new[c, k] = was["prim"][5 + c][0] - COURANT * curls[c]
            for i, (here_at, there) in enumerate(((conserved, conserved_out), (faces_new, faces_out))):
                copy = pltpu.make_async_copy(here_at.at[:, k], there.at[:, k], sems.at[2 * k + i])
                copy.start()
                copies.append(copy)
        previous = now
    for copy in copies:
        copy.wait()


VMEM = pl.BlockSpec(memory_space=pltpu.VMEM)
SMEM = pl.BlockSpec(memory_space=pltpu.SMEM)


def shape(*dims):
    return jax.ShapeDtypeStruct(dims, f32)


def held(*dims):
    return pltpu.VMEM(dims, f32)


def near(*arrays):
    return [pltpu.with_memory_space_constraint(a, pltpu.VMEM) for a in arrays]


def neighbours(axis):
    count = lax.axis_size(axis)
    return [(i, i + 1) for i in range(count - 1)], [(i + 1, i) for i in range(count - 1)]


def on_device(density, velocity, pressure, field, corona):
    own, top, bottom = pl.pallas_call(
        gather_block,
        out_shape=(held(8, NZ, NY, NX), held(8, NY, NX), held(9, NY, NX)),
        in_specs=[pl.BlockSpec(memory_space=pl.ANY)] * 4,
        out_specs=(VMEM,) * 3,
        scratch_shapes=[pltpu.SemaphoreType.DMA((13,))],
        name="gather_block",
    )(density, velocity, pressure, field)
    up, down = neighbours("gz")
    below = lax.ppermute(top, "gz", up)
    above = lax.ppermute(bottom, "gz", down)
    rows_up, rows_down = pl.pallas_call(
        pack_rows,
        out_shape=(held(UP_ROWS, NX), held(DOWN_ROWS, NX)),
        in_specs=[VMEM] * 3,
        out_specs=(VMEM, VMEM),
        name="pack_rows",
    )(*near(own, below, above))
    up, down = neighbours("gy")
    left_rows = lax.ppermute(rows_up, "gy", up)
    right_rows = lax.ppermute(rows_down, "gy", down)
    main, main_cols = pl.pallas_call(
        pack_main,
        out_shape=(held(8, 11, 8, NX), held(3, 8, NX)),
        in_specs=[SMEM] + [VMEM] * 3,
        out_specs=(VMEM, VMEM),
        name="pack_main",
    )(corona, *near(own, below, above))
    edges, cols = pl.pallas_call(
        pack_edges,
        out_shape=(held(8, 11, 8, NX), held(3, 16, NX)),
        in_specs=[SMEM] + [VMEM] * 4,
        out_specs=(VMEM, VMEM),
        name="pack_edges",
    )(corona, *near(main, main_cols, left_rows, right_rows))
    gathered = lax.all_gather(cols, "gx", axis=0)
    return pl.pallas_call(
        advance,
        out_shape=(shape(5, NZ, NY, NX), shape(3, NZ, NY, NX)),
        in_specs=[VMEM] * 4,
        out_specs=(pl.BlockSpec(memory_space=pl.ANY),) * 2,
        scratch_shapes=[
            pltpu.VMEM((5, NZ, NY, NX), f32),
            pltpu.VMEM((3, NZ, NY, NX), f32),
            pltpu.SemaphoreType.DMA((2 * NZ,)),
        ],
        name="advance",
    )(*near(gathered, cols, main, edges))


def solution(mesh):
    block = P("gz", "gy", "gx")
    blocks = P(None, "gz", "gy", "gx")
    return jax.shard_map(
        on_device,
        mesh=mesh,
        in_specs=(block, blocks, block, blocks, P()),
        out_specs=(blocks, blocks),
        check_vma=False,
    )
```

```python
import jax
import jax.numpy as jnp
from jax import lax
from jax.experimental import pallas as pl
from jax.experimental.pallas import tpu as pltpu
from jax.sharding import PartitionSpec as P


COOL_STEPS = 8
GAMMA = 5.0 / 3.0
COURANT = 0.08
COOL_RATE = 0.03
GRAVITY = 1.0

NZ, NY, NX = 8, 8, 128
ROWS = 10
UP_ROWS, DOWN_ROWS = 88, 96
Z_MAIN = range(NZ)

f32 = jnp.float32


def gather_block(density, velocity, pressure, field, corona, own, top, bottom, marks, mask, sems):
    one = pl.ds(0, 1)
    copies = []
    for out, z in ((top, NZ - 1), (bottom, 0)):
        copies += [
            (density.at[pl.ds(z, 1)], out.at[one]),
            (velocity.at[:, z], out.at[pl.ds(1, 3)]),
            (pressure.at[pl.ds(z, 1)], out.at[pl.ds(4, 1)]),
            (field.at[:, z], out.at[pl.ds(5, 3)]),
        ]
    copies += [
        (field.at[0, pl.ds(1, 1)], bottom.at[pl.ds(8, 1)]),
        (density, own.at[0]),
        (velocity, own.at[pl.ds(1, 3)]),
        (pressure, own.at[4]),
        (field, own.at[pl.ds(5, 3)]),
        (corona, mask),
    ]
    copies = [pltpu.make_async_copy(a, b, sems.at[i]) for i, (a, b) in enumerate(copies)]
    for copy in copies:
        copy.start()
    for copy in copies:
        copy.wait()
    first, last = lax.axis_index("gz") * NZ, lax.axis_size("gz") * NZ - 1
    for z in range(ROWS):
        marks[z] = jnp.full((8, NX), mask[jnp.clip(first + z - 1, 0, last)], jnp.int32)


def pack_rows(own, below, above, up, down):
    lowest = lax.axis_index("gz") == 0
    highest = lax.axis_index("gz") == lax.axis_size("gz") - 1

    def put(out, at, row):
        out[pl.ds(at, 1), :] = row

    for out, y in ((up, NY - 1), (down, 0)):
        for member in range(8):
            base = member * ROWS
            for z in Z_MAIN:
                put(out, base + 1 + z, own[member, z, pl.ds(y, 1), :])
            put(out, base, below[member, pl.ds(y, 1), :])
            put(out, base + 9, above[member, pl.ds(y, 1), :])
        put(out, 80, above[8, pl.ds(y, 1), :])
    for z in Z_MAIN:
        put(down, 82 + z, own[6, z, pl.ds(1, 1), :])
    put(down, 81, below[6, pl.ds(1, 1), :])
    put(down, 90, above[6, pl.ds(1, 1), :])

    @pl.when(lowest)
    def _():
        for out, y in ((up, NY - 1), (down, 0)):
            for member in range(8):
                put(out, member * ROWS, own[member, 0, pl.ds(y, 1), :])
        put(down, 81, own[6, 0, pl.ds(1, 1), :])

    @pl.when(highest)
    def _():
        for out, y in ((up, NY - 1), (down, 0)):
            for member in range(8):
                put(out, member * ROWS + 9, own[member, NZ - 1, pl.ds(y, 1), :])
            put(out, 80, own[5, NZ - 1, pl.ds(y, 1), :])
        put(down, 90, own[6, NZ - 1, pl.ds(1, 1), :])


def lanes():
    return lax.broadcasted_iota(jnp.int32, (8, NX), 1)


def sublanes():
    return lax.broadcasted_iota(jnp.int32, (8, NX), 0)


def roll(values, by, axis):
    size = values.shape[axis]
    by = by % size
    return values if by == 0 else pltpu.roll(values, by, axis)


def cool(marks, ext):
    rho = [ext[0, z] for z in range(ROWS)]
    raw = [ext[4, z] for z in range(ROWS)]
    now = list(raw)
    for _ in range(COOL_STEPS):
        now = [p / (1.0 + COOL_RATE * root(r * p)) for r, p in zip(rho, now)]
    for z, (p, q) in enumerate(zip(raw, now)):
        ext[4, z] = jnp.where(marks[z] == 1, q, p)


def columns_of(ext):
    lane = lanes()
    low = high = second = jnp.zeros((8, NX), f32)
    for z in range(11):
        for member in range(8) if z < 10 else (5,):
            at = 8 * z + member
            tile = ext[member, z]
            low = jnp.where(lane == at, roll(tile, at, 1), low)
            high = jnp.where(lane == at, roll(tile, at + 1, 1), high)
            if member == 7:
                second = jnp.where(lane == 8 * z + 2, roll(tile, 8 * z + 1, 1), second)
    return low, high, second


def pack_main(marks, own, below, above, ext, cols):
    slab_at, slab_count = lax.axis_index("gz"), lax.axis_size("gz")
    for member in range(8):
        for z in Z_MAIN:
            ext[member, z + 1] = own[member, z]
        ext[member, 0] = below[member]
        ext[member, 9] = above[member]
    ext[5, 10] = above[8]

    @pl.when(slab_at == 0)
    def _():
        for member in range(8):
            ext[member, 0] = own[member, 0]

    @pl.when(slab_at == slab_count - 1)
    def _():
        for member in range(8):
            ext[member, 9] = own[member, NZ - 1]
        ext[5, 10] = own[5, NZ - 1]

    cool(marks, ext)
    for i, v in enumerate(columns_of(ext)):
        cols[i] = v


PLACES = [(member, z, member * ROWS + z) for member in range(8) for z in range(ROWS)] + [(5, 10, 80)]


def pack_edges(marks, main, main_cols, left_rows, right_rows, ext, cols):
    row_at, row_count = lax.axis_index("gy"), lax.axis_size("gy")
    for member, z, at in PLACES:
        ext[member, z, 7:8, :] = left_rows[pl.ds(at, 1), :]
        ext[member, z, 0:1, :] = right_rows[pl.ds(at, 1), :]
    for z in range(ROWS):
        ext[6, z, 1:2, :] = right_rows[pl.ds(81 + z, 1), :]
    cool(marks, ext)

    @pl.when(row_at == 0)
    def _():
        for member, z, _at in PLACES:
            ext[member, z, 7:8, :] = main[member, z, 0:1, :]

    @pl.when(row_at == row_count - 1)
    def _():
        for member, z, _at in PLACES:
            ext[member, z, 0:1, :] = main[member, z, 7:8, :]
        for z in range(ROWS):
            ext[6, z, 1:2, :] = main[6, z, 7:8, :]

    for i, v in enumerate(columns_of(ext)):
        cols[i, 0:8, :] = main_cols[i]
        cols[i, 8:16, :] = v


class Cell:
    def __init__(self, rho, vel, p, cen):
        self.rho, self.vel, self.p, self.cen = rho, vel, p, cen
        self.mom = [rho * v for v in vel]
        kinetic = self.mom[0] * vel[0] + self.mom[1] * vel[1] + self.mom[2] * vel[2]
        self.thermal = p * (1.0 / (GAMMA - 1.0)) + 0.5 * kinetic
        self.inv = 1.0 / rho
        self.sound = GAMMA * p * self.inv


def root(x):
    return x * lax.rsqrt(x)


def speeds(cell, square, axis):
    b, c = [k for k in range(3) if k != axis]
    across = cell.cen[b] * cell.cen[b] + cell.cen[c] * cell.cen[c]
    n, t, s = square * cell.inv, across * cell.inv, cell.sound
    gap = s - n - t
    inner = root(jnp.maximum(gap * gap + 4.0 * s * t, 1e-30))
    return across, root(0.5 * (s + n + t + inner))


def side(cell, normal, square, across, axis, speed, weight, member):
    vel, cen, va = cell.vel, cell.cen, cell.vel[axis]
    w, wn = weight * (va - speed), weight * normal
    if member == 0:
        return cell.rho * w
    if member == axis + 1:
        return cell.mom[axis] * w + weight * (cell.p + 0.5 * (across - square))
    if member < 4:
        return cell.mom[member - 1] * w - cen[member - 1] * wn
    b, c = [k for k in range(3) if k != axis]
    if member == 4:
        half = 0.5 * (across + square)
        align = va * normal + vel[b] * cen[b] + vel[c] * cen[c]
        return (cell.thermal + half) * w + weight * ((cell.p + half) * va - normal * align)
    k = (b, c)[member - 5]
    return cen[k] * w - vel[k] * wn


def hll(lower, upper, normal, axis, members):
    square = normal * normal
    la, lf = speeds(lower, square, axis)
    ua, uf = speeds(upper, square, axis)
    lv, uv = lower.vel[axis], upper.vel[axis]
    slow = jnp.minimum(jnp.minimum(lv - lf, uv - uf), 0.0)
    fast = jnp.maximum(jnp.maximum(lv + lf, uv + uf), 0.0)
    inverse = 1.0 / (fast - slow)
    a, b = fast * inverse, slow * inverse
    return {
        m: side(lower, normal, square, la, axis, slow, a, m) - side(upper, normal, square, ua, axis, fast, b, m)
        for m in members
    }


def member_of(axis, component):
    return 5 + [k for k in range(3) if k != axis].index(component)


def advance(gathered, own_cols, main, edges, conserved_out, faces_out, conserved, faces_new, sems):
    lane, sub = lanes(), sublanes()
    size = lax.axis_size("gx")
    at = lax.axis_index("gx")
    left, right = lax.rem(at + size - 1, size), lax.rem(at + 1, size)
    first_lane, last_lane = lane == 0, lane == NX - 1
    first_row, last_row = sub == 0, sub == 7
    slot = lane % 8

    def down_y(q):
        r0, r1 = roll(q[0], 1, 0), roll(q[1], 1, 0)
        return [jnp.where(first_row, r1, r0), jnp.where(first_row, r0, r1)]

    def up_y(q):
        r0, r1 = roll(q[0], -1, 0), roll(q[1], -1, 0)
        return [jnp.where(last_row, r1, r0), jnp.where(last_row, r0, r1)]

    def down_x(q, side, source):
        return jnp.where(first_lane, roll(side, -source, 1), roll(q, 1, 1))

    def up_x(q, side, source):
        return jnp.where(last_lane, roll(side, NX - 1 - source, 1), roll(q, -1, 1))

    low_r = [gathered[right, 0, 8 * t : 8 * t + 8, :] for t in range(2)]
    two_r = [gathered[right, 2, 8 * t : 8 * t + 8, :] for t in range(2)]
    high_l = [gathered[left, 1, 8 * t : 8 * t + 8, :] for t in range(2)]
    own_low = [own_cols[0, 8 * t : 8 * t + 8, :] for t in range(2)]
    own_high = [own_cols[1, 8 * t : 8 * t + 8, :] for t in range(2)]

    def column(member):
        out = []
        for t in range(2):
            v = roll(own_high[t], -member, 1)
            v = jnp.where(slot == 1, roll(low_r[t], 1 - member, 1), v)
            v = jnp.where(slot == 3, roll(high_l[t], 3 - member, 1), v)
            v = jnp.where(slot == 4, roll(own_low[t], 4 - member, 1), v)
            if member == 7:
                v = jnp.where(slot == 2, two_r[t], v)
            out.append(v)
        return out

    col = [column(member) for member in range(8)]
    col_next_y = up_y(col[6])
    col_cen = [
        [0.5 * (v + roll(v, -8, 1)) for v in col[5]],
        [0.5 * (v + n) for v, n in zip(col[6], col_next_y)],
        [0.5 * (v + roll(v, -1, 1)) for v in col[7]],
    ]

    def cells(prim, cen):
        return [Cell(prim[0][t], [prim[k][t] for k in (1, 2, 3)], prim[4][t], [cen[k][t] for k in range(3)]) for t in range(2)]

    col_cell = cells(col, col_cen)
    shifted = lambda by: cells(
        [[roll(v, by, 1) for v in col[k]] for k in range(5)],
        [[roll(v, by, 1) for v in col_cen[k]] for k in range(3)],
    )
    full = tuple(range(7))
    col_x_lower, col_z_lower = shifted(1), shifted(8)
    col_y_lower = cells([down_y(col[k]) for k in range(5)], [down_y(col_cen[k]) for k in range(3)])
    XB = {(a, k): member_of(a, k) for a in range(3) for k in range(3) if a != k}
    col_fx = [hll(col_x_lower[0], col_cell[0], col[7][0], 2, full), hll(col_x_lower[1], col_cell[1], col[7][1], 2, (XB[2, 1],))]
    col_fy = [hll(col_y_lower[t], col_cell[t], col[6][t], 1, (XB[1, 2],))[XB[1, 2]] for t in range(2)]
    col_fz = hll(col_z_lower[0], col_cell[0], col[5][0], 0, (XB[0, 2],))[XB[0, 2]]
    fx_by = [f[XB[2, 1]] for f in col_fx]
    fx_bz = col_fx[0][XB[2, 0]]
    down = down_y(fx_by)
    col_ez = [0.25 * (col_fy[t] + roll(col_fy[t], 1, 1) - fx_by[t] - down[t]) for t in range(2)]
    col_ey = 0.25 * (fx_bz + roll(fx_bz, 8, 1) - col_fz - roll(col_fz, 1, 1))

    def slab_cells(z):
        base = 8 * (z + 1)
        get = lambda member, s: [main[member, s], edges[member, s]]
        prim = [get(member, z + 1) for member in range(8)]
        next_z = get(5, z + 2)
        next_y = up_y(prim[6])
        next_x = [up_x(prim[7][t], low_r[t], base + 7) for t in range(2)]
        cen = [
            [0.5 * (prim[5][t] + next_z[t]) for t in range(2)],
            [0.5 * (prim[6][t] + next_y[t]) for t in range(2)],
            [0.5 * (prim[7][t] + next_x[t]) for t in range(2)],
        ]
        return prim, cen, cells(prim, cen)

    def slab_fluxes(z, prim, cen, here, below):
        base = 8 * (z + 1)
        inside = 0 <= z < NZ
        fz = fy = fx = None
        if z >= 0:
            fz = [
                hll(below[0], here[0], prim[5][0], 0, full),
                hll(below[1], here[1], prim[5][1], 0, (XB[0, 1],)),
            ]
        y_lower = cells([down_y(prim[k]) for k in range(5)], [down_y(cen[k]) for k in range(3)])
        x_lower = []
        for t in range(2):
            p = [down_x(prim[k][t], high_l[t], base + k) for k in range(5)]
            c = [down_x(cen[k][t], col_cen[k][t], base + 3) for k in range(3)]
            x_lower.append(Cell(p[0], p[1:4], p[4], c))
        members = full if inside else (XB[1, 0],)
        fy = [hll(y_lower[t], here[t], prim[6][t], 1, members) for t in range(2)]
        if inside:
            fx = [
                hll(x_lower[0], here[0], prim[7][0], 2, full),
                hll(x_lower[1], here[1], prim[7][1], 2, (XB[2, 1],)),
            ]
        else:
            fx = [hll(x_lower[0], here[0], prim[7][0], 2, (XB[2, 0],)), None]
        return fz, fy, fx

    slabs = lax.axis_size("gz") * NZ
    first_slab = lax.axis_index("gz") * NZ
    previous = None
    copies = []
    for z in range(-1, NZ + 1):
        base = 8 * (z + 1)
        prim, cen, here = slab_cells(z)
        below = previous["here"] if previous else None
        fz, fy, fx = slab_fluxes(z, prim, cen, here, below)
        now = dict(prim=prim, cen=cen, here=here, fz=fz, fy=fy, fx=fx, base=base)
        if z >= 0:
            by = [fz[t][XB[0, 1]] for t in range(2)]
            by_down = down_y(by)
            now["ex"] = [0.25 * (by[t] + by_down[t] - fy[t][XB[1, 0]] - previous["fy"][t][XB[1, 0]]) for t in range(2)]
            bx = fz[0][XB[0, 2]]
            now["ey"] = 0.25 * (fx[0][XB[2, 0]] + previous["fx"][0][XB[2, 0]] - bx - down_x(bx, col_fz, base + 3))
        if 0 <= z < NZ:
            bx = [fy[t][XB[1, 2]] for t in range(2)]
            by = [fx[t][XB[2, 1]] for t in range(2)]
            by_down = down_y(by)
            now["ez"] = [0.25 * (bx[t] + down_x(bx[t], col_fy[t], base + 3) - by[t] - by_down[t]) for t in range(2)]
        if z >= 1:
            k = z - 1
            was = previous
            cell = was["here"][0]
            pull = -GRAVITY * (2 * (first_slab + k) + 1 - slabs).astype(f32) / slabs
            squared = sum(c[0] * c[0] for c in was["cen"])
            held = [cell.rho] + cell.mom + [cell.thermal + 0.5 * squared]
            for m in range(5):
                y_next = up_y([was["fy"][t][m] for t in range(2)])[0]
                x_next = up_x(was["fx"][0][m], col_fx[0][m], was["base"] + 1)
                change = (fz[0][m] - was["fz"][0][m]) + (y_next - was["fy"][0][m]) + (x_next - was["fx"][0][m])
                value = held[m] - COURANT * change
                if m == 1:
                    value = value + (COURANT * pull) * cell.rho
                if m == 4:
                    value = value + (COURANT * pull) * cell.mom[0]
                conserved[m, k] = value
            ex, ey, ez = was["ex"], was["ey"], was["ez"]
            ex_up_y, ez_up_y = up_y(ex)[0], up_y(ez)[0]
            ey_up_x = up_x(ey, col_ey, was["base"] + 1)
            ez_up_x = up_x(ez[0], col_ez[0], was["base"] + 1)
            curls = (
                ey_up_x - ey - (ex_up_y - ex[0]),
                now["ex"][0] - ex[0] - (ez_up_x - ez[0]),
                ez_up_y - ez[0] - (now["ey"] - ey),
            )
            for c in range(3):
                faces_new[c, k] = was["prim"][5 + c][0] - COURANT * curls[c]
            for i, (here_at, there) in enumerate(((conserved, conserved_out), (faces_new, faces_out))):
                copy = pltpu.make_async_copy(here_at.at[:, k], there.at[:, k], sems.at[2 * k + i])
                copy.start()
                copies.append(copy)
        previous = now
    for copy in copies:
        copy.wait()


VMEM = pl.BlockSpec(memory_space=pltpu.VMEM)


def shape(*dims):
    return jax.ShapeDtypeStruct(dims, f32)


def held(*dims, dtype=f32):
    return pltpu.VMEM(dims, dtype)


def near(*arrays):
    return [pltpu.with_memory_space_constraint(a, pltpu.VMEM) for a in arrays]


def neighbours(axis):
    count = lax.axis_size(axis)
    return [(i, i + 1) for i in range(count - 1)], [(i + 1, i) for i in range(count - 1)]


def on_device(density, velocity, pressure, field, corona):
    own, top, bottom, marks = pl.pallas_call(
        gather_block,
        out_shape=(held(8, NZ, NY, NX), held(8, NY, NX), held(9, NY, NX), held(ROWS, NY, NX, dtype=jnp.int32)),
        in_specs=[pl.BlockSpec(memory_space=pl.ANY)] * 5,
        out_specs=(VMEM,) * 4,
        scratch_shapes=[pltpu.SMEM(corona.shape, jnp.int32), pltpu.SemaphoreType.DMA((14,))],
        name="gather_block",
    )(density, velocity, pressure, field, corona)
    up, down = neighbours("gz")
    below = lax.ppermute(top, "gz", up)
    above = lax.ppermute(bottom, "gz", down)
    rows_up, rows_down = pl.pallas_call(
        pack_rows,
        out_shape=(held(UP_ROWS, NX), held(DOWN_ROWS, NX)),
        in_specs=[VMEM] * 3,
        out_specs=(VMEM, VMEM),
        name="pack_rows",
    )(*near(own, below, above))
    up, down = neighbours("gy")
    left_rows = lax.ppermute(rows_up, "gy", up)
    right_rows = lax.ppermute(rows_down, "gy", down)
    main, main_cols = pl.pallas_call(
        pack_main,
        out_shape=(held(8, 11, 8, NX), held(3, 8, NX)),
        in_specs=[VMEM] * 4,
        out_specs=(VMEM, VMEM),
        name="pack_main",
    )(*near(marks, own, below, above))
    edges, cols = pl.pallas_call(
        pack_edges,
        out_shape=(held(8, 11, 8, NX), held(3, 16, NX)),
        in_specs=[VMEM] * 5,
        out_specs=(VMEM, VMEM),
        name="pack_edges",
    )(*near(marks, main, main_cols, left_rows, right_rows))
    gathered = lax.all_gather(cols, "gx", axis=0)
    return pl.pallas_call(
        advance,
        out_shape=(shape(5, NZ, NY, NX), shape(3, NZ, NY, NX)),
        in_specs=[VMEM] * 4,
        out_specs=(pl.BlockSpec(memory_space=pl.ANY),) * 2,
        scratch_shapes=[
            pltpu.VMEM((5, NZ, NY, NX), f32),
            pltpu.VMEM((3, NZ, NY, NX), f32),
            pltpu.SemaphoreType.DMA((2 * NZ,)),
        ],
        name="advance",
    )(*near(gathered, cols, main, edges))


def solution(mesh):
    block = P("gz", "gy", "gx")
    blocks = P(None, "gz", "gy", "gx")
    return jax.shard_map(
        on_device,
        mesh=mesh,
        in_specs=(block, blocks, block, blocks, P()),
        out_specs=(blocks, blocks),
        check_vma=False,
    )
```

```python
import jax
import jax.numpy as jnp
from jax import lax
from jax.experimental import pallas as pl
from jax.experimental.pallas import tpu as pltpu
from jax.sharding import PartitionSpec as P


COOL_STEPS = 8
GAMMA = 5.0 / 3.0
COURANT = 0.08
COOL_RATE = 0.03
GRAVITY = 1.0

NZ, NY, NX = 8, 8, 128
ROWS = 10
UP_ROWS, DOWN_ROWS = 88, 96
Z_MAIN = range(NZ)

f32 = jnp.float32


def run_copies(pairs, sems):
    copies = [pltpu.make_async_copy(a, b, sems.at[i]) for i, (a, b) in enumerate(pairs)]
    for copy in copies:
        copy.start()
    for copy in copies:
        copy.wait()


def gather_layers(density, velocity, pressure, field, top, bottom, sems):
    one = pl.ds(0, 1)
    pairs = [(field.at[0, pl.ds(1, 1)], bottom.at[pl.ds(8, 1)])]
    for out, z in ((top, NZ - 1), (bottom, 0)):
        pairs += [
            (density.at[pl.ds(z, 1)], out.at[one]),
            (velocity.at[:, z], out.at[pl.ds(1, 3)]),
            (pressure.at[pl.ds(z, 1)], out.at[pl.ds(4, 1)]),
            (field.at[:, z], out.at[pl.ds(5, 3)]),
        ]
    run_copies(pairs, sems)


def gather_block(density, velocity, pressure, field, corona, own, marks, mask, sems):
    pairs = [
        (density, own.at[0]),
        (velocity, own.at[pl.ds(1, 3)]),
        (pressure, own.at[4]),
        (field, own.at[pl.ds(5, 3)]),
        (corona, mask),
    ]
    run_copies(pairs, sems)
    first, last = lax.axis_index("gz") * NZ, lax.axis_size("gz") * NZ - 1
    for z in range(ROWS):
        marks[z] = jnp.full((8, NX), mask[jnp.clip(first + z - 1, 0, last)], jnp.int32)


def pack_rows(own, below, above, up, down):
    lowest = lax.axis_index("gz") == 0
    highest = lax.axis_index("gz") == lax.axis_size("gz") - 1

    def put(out, at, row):
        out[pl.ds(at, 1), :] = row

    for out, y in ((up, NY - 1), (down, 0)):
        for member in range(8):
            base = member * ROWS
            for z in Z_MAIN:
                put(out, base + 1 + z, own[member, z, pl.ds(y, 1), :])
            put(out, base, below[member, pl.ds(y, 1), :])
            put(out, base + 9, above[member, pl.ds(y, 1), :])
        put(out, 80, above[8, pl.ds(y, 1), :])
    for z in Z_MAIN:
        put(down, 82 + z, own[6, z, pl.ds(1, 1), :])
    put(down, 81, below[6, pl.ds(1, 1), :])
    put(down, 90, above[6, pl.ds(1, 1), :])

    @pl.when(lowest)
    def _():
        for out, y in ((up, NY - 1), (down, 0)):
            for member in range(8):
                put(out, member * ROWS, own[member, 0, pl.ds(y, 1), :])
        put(down, 81, own[6, 0, pl.ds(1, 1), :])

    @pl.when(highest)
    def _():
        for out, y in ((up, NY - 1), (down, 0)):
            for member in range(8):
                put(out, member * ROWS + 9, own[member, NZ - 1, pl.ds(y, 1), :])
            put(out, 80, own[5, NZ - 1, pl.ds(y, 1), :])
        put(down, 90, own[6, NZ - 1, pl.ds(1, 1), :])


def lanes():
    return lax.broadcasted_iota(jnp.int32, (8, NX), 1)


def sublanes():
    return lax.broadcasted_iota(jnp.int32, (8, NX), 0)


def roll(values, by, axis):
    size = values.shape[axis]
    by = by % size
    return values if by == 0 else pltpu.roll(values, by, axis)


def cool(marks, ext):
    rho = [ext[0, z] for z in range(ROWS)]
    raw = [ext[4, z] for z in range(ROWS)]
    now = list(raw)
    for _ in range(COOL_STEPS):
        now = [p / (1.0 + COOL_RATE * root(r * p)) for r, p in zip(rho, now)]
    for z, (p, q) in enumerate(zip(raw, now)):
        ext[4, z] = jnp.where(marks[z] == 1, q, p)


def columns_of(ext):
    lane = lanes()
    low = high = second = jnp.zeros((8, NX), f32)
    for z in range(11):
        for member in range(8) if z < 10 else (5,):
            at = 8 * z + member
            tile = ext[member, z]
            low = jnp.where(lane == at, roll(tile, at, 1), low)
            high = jnp.where(lane == at, roll(tile, at + 1, 1), high)
            if member == 7:
                second = jnp.where(lane == 8 * z + 2, roll(tile, 8 * z + 1, 1), second)
    return low, high, second


def pack_main(marks, own, below, above, ext, cols):
    slab_at, slab_count = lax.axis_index("gz"), lax.axis_size("gz")
    for member in range(8):
        for z in Z_MAIN:
            ext[member, z + 1] = own[member, z]
        ext[member, 0] = below[member]
        ext[member, 9] = above[member]
    ext[5, 10] = above[8]

    @pl.when(slab_at == 0)
    def _():
        for member in range(8):
            ext[member, 0] = own[member, 0]

    @pl.when(slab_at == slab_count - 1)
    def _():
        for member in range(8):
            ext[member, 9] = own[member, NZ - 1]
        ext[5, 10] = own[5, NZ - 1]

    cool(marks, ext)
    for i, v in enumerate(columns_of(ext)):
        cols[i] = v


PLACES = [(member, z, member * ROWS + z) for member in range(8) for z in range(ROWS)] + [(5, 10, 80)]


def pack_edges(marks, main, main_cols, left_rows, right_rows, ext, cols):
    row_at, row_count = lax.axis_index("gy"), lax.axis_size("gy")
    for member, z, at in PLACES:
        ext[member, z, 7:8, :] = left_rows[pl.ds(at, 1), :]
        ext[member, z, 0:1, :] = right_rows[pl.ds(at, 1), :]
    for z in range(ROWS):
        ext[6, z, 1:2, :] = right_rows[pl.ds(81 + z, 1), :]
    cool(marks, ext)

    @pl.when(row_at == 0)
    def _():
        for member, z, _at in PLACES:
            ext[member, z, 7:8, :] = main[member, z, 0:1, :]

    @pl.when(row_at == row_count - 1)
    def _():
        for member, z, _at in PLACES:
            ext[member, z, 0:1, :] = main[member, z, 7:8, :]
        for z in range(ROWS):
            ext[6, z, 1:2, :] = main[6, z, 7:8, :]

    for i, v in enumerate(columns_of(ext)):
        cols[i, 0:8, :] = main_cols[i]
        cols[i, 8:16, :] = v


class Cell:
    def __init__(self, rho, vel, p, cen):
        self.rho, self.vel, self.p, self.cen = rho, vel, p, cen
        self.mom = [rho * v for v in vel]
        kinetic = self.mom[0] * vel[0] + self.mom[1] * vel[1] + self.mom[2] * vel[2]
        self.thermal = p * (1.0 / (GAMMA - 1.0)) + 0.5 * kinetic
        self.inv = 1.0 / rho
        self.sound = GAMMA * p * self.inv


def root(x):
    return x * lax.rsqrt(x)


def speeds(cell, square, axis):
    b, c = [k for k in range(3) if k != axis]
    across = cell.cen[b] * cell.cen[b] + cell.cen[c] * cell.cen[c]
    n, t, s = square * cell.inv, across * cell.inv, cell.sound
    gap = s - n - t
    inner = root(jnp.maximum(gap * gap + 4.0 * s * t, 1e-30))
    return across, root(0.5 * (s + n + t + inner))


def side(cell, normal, square, across, axis, speed, weight, member):
    vel, cen, va = cell.vel, cell.cen, cell.vel[axis]
    w, wn = weight * (va - speed), weight * normal
    if member == 0:
        return cell.rho * w
    if member == axis + 1:
        return cell.mom[axis] * w + weight * (cell.p + 0.5 * (across - square))
    if member < 4:
        return cell.mom[member - 1] * w - cen[member - 1] * wn
    b, c = [k for k in range(3) if k != axis]
    if member == 4:
        half = 0.5 * (across + square)
        align = va * normal + vel[b] * cen[b] + vel[c] * cen[c]
        return (cell.thermal + half) * w + weight * ((cell.p + half) * va - normal * align)
    k = (b, c)[member - 5]
    return cen[k] * w - vel[k] * wn


def hll(lower, upper, normal, axis, members):
    square = normal * normal
    la, lf = speeds(lower, square, axis)
    ua, uf = speeds(upper, square, axis)
    lv, uv = lower.vel[axis], upper.vel[axis]
    slow = jnp.minimum(jnp.minimum(lv - lf, uv - uf), 0.0)
    fast = jnp.maximum(jnp.maximum(lv + lf, uv + uf), 0.0)
    inverse = 1.0 / (fast - slow)
    a, b = fast * inverse, slow * inverse
    return {
        m: side(lower, normal, square, la, axis, slow, a, m) - side(upper, normal, square, ua, axis, fast, b, m)
        for m in members
    }


def member_of(axis, component):
    return 5 + [k for k in range(3) if k != axis].index(component)


def advance(gathered, own_cols, main, edges, conserved_out, faces_out, conserved, faces_new, sems):
    lane, sub = lanes(), sublanes()
    size = lax.axis_size("gx")
    at = lax.axis_index("gx")
    left, right = lax.rem(at + size - 1, size), lax.rem(at + 1, size)
    first_lane, last_lane = lane == 0, lane == NX - 1
    first_row, last_row = sub == 0, sub == 7
    slot = lane % 8

    def down_y(q):
        r0, r1 = roll(q[0], 1, 0), roll(q[1], 1, 0)
        return [jnp.where(first_row, r1, r0), jnp.where(first_row, r0, r1)]

    def up_y(q):
        r0, r1 = roll(q[0], -1, 0), roll(q[1], -1, 0)
        return [jnp.where(last_row, r1, r0), jnp.where(last_row, r0, r1)]

    def down_x(q, side, source):
        return jnp.where(first_lane, roll(side, -source, 1), roll(q, 1, 1))

    def up_x(q, side, source):
        return jnp.where(last_lane, roll(side, NX - 1 - source, 1), roll(q, -1, 1))

    low_r = [gathered[right, 0, 8 * t : 8 * t + 8, :] for t in range(2)]
    two_r = [gathered[right, 2, 8 * t : 8 * t + 8, :] for t in range(2)]
    high_l = [gathered[left, 1, 8 * t : 8 * t + 8, :] for t in range(2)]
    own_low = [own_cols[0, 8 * t : 8 * t + 8, :] for t in range(2)]
    own_high = [own_cols[1, 8 * t : 8 * t + 8, :] for t in range(2)]

    def column(member):
        out = []
        for t in range(2):
            v = roll(own_high[t], -member, 1)
            v = jnp.where(slot == 1, roll(low_r[t], 1 - member, 1), v)
            v = jnp.where(slot == 3, roll(high_l[t], 3 - member, 1), v)
            v = jnp.where(slot == 4, roll(own_low[t], 4 - member, 1), v)
            if member == 7:
                v = jnp.where(slot == 2, two_r[t], v)
            out.append(v)
        return out

    col = [column(member) for member in range(8)]
    col_next_y = up_y(col[6])
    col_cen = [
        [0.5 * (v + roll(v, -8, 1)) for v in col[5]],
        [0.5 * (v + n) for v, n in zip(col[6], col_next_y)],
        [0.5 * (v + roll(v, -1, 1)) for v in col[7]],
    ]

    def cells(prim, cen):
        return [Cell(prim[0][t], [prim[k][t] for k in (1, 2, 3)], prim[4][t], [cen[k][t] for k in range(3)]) for t in range(2)]

    col_cell = cells(col, col_cen)
    shifted = lambda by: cells(
        [[roll(v, by, 1) for v in col[k]] for k in range(5)],
        [[roll(v, by, 1) for v in col_cen[k]] for k in range(3)],
    )
    full = tuple(range(7))
    col_x_lower, col_z_lower = shifted(1), shifted(8)
    col_y_lower = cells([down_y(col[k]) for k in range(5)], [down_y(col_cen[k]) for k in range(3)])
    XB = {(a, k): member_of(a, k) for a in range(3) for k in range(3) if a != k}
    col_fx = [hll(col_x_lower[0], col_cell[0], col[7][0], 2, full), hll(col_x_lower[1], col_cell[1], col[7][1], 2, (XB[2, 1],))]
    col_fy = [hll(col_y_lower[t], col_cell[t], col[6][t], 1, (XB[1, 2],))[XB[1, 2]] for t in range(2)]
    col_fz = hll(col_z_lower[0], col_cell[0], col[5][0], 0, (XB[0, 2],))[XB[0, 2]]
    fx_by = [f[XB[2, 1]] for f in col_fx]
    fx_bz = col_fx[0][XB[2, 0]]
    down = down_y(fx_by)
    col_ez = [0.25 * (col_fy[t] + roll(col_fy[t], 1, 1) - fx_by[t] - down[t]) for t in range(2)]
    col_ey = 0.25 * (fx_bz + roll(fx_bz, 8, 1) - col_fz - roll(col_fz, 1, 1))

    def slab_cells(z):
        base = 8 * (z + 1)
        get = lambda member, s: [main[member, s], edges[member, s]]
        prim = [get(member, z + 1) for member in range(8)]
        next_z = get(5, z + 2)
        next_y = up_y(prim[6])
        next_x = [up_x(prim[7][t], low_r[t], base + 7) for t in range(2)]
        cen = [
            [0.5 * (prim[5][t] + next_z[t]) for t in range(2)],
            [0.5 * (prim[6][t] + next_y[t]) for t in range(2)],
            [0.5 * (prim[7][t] + next_x[t]) for t in range(2)],
        ]
        return prim, cen, cells(prim, cen)

    def slab_fluxes(z, prim, cen, here, below):
        base = 8 * (z + 1)
        inside = 0 <= z < NZ
        fz = fy = fx = None
        if z >= 0:
            fz = [
                hll(below[0], here[0], prim[5][0], 0, full),
                hll(below[1], here[1], prim[5][1], 0, (XB[0, 1],)),
            ]
        y_lower = cells([down_y(prim[k]) for k in range(5)], [down_y(cen[k]) for k in range(3)])
        x_lower = []
        for t in range(2):
            p = [down_x(prim[k][t], high_l[t], base + k) for k in range(5)]
            c = [down_x(cen[k][t], col_cen[k][t], base + 3) for k in range(3)]
            x_lower.append(Cell(p[0], p[1:4], p[4], c))
        members = full if inside else (XB[1, 0],)
        fy = [hll(y_lower[t], here[t], prim[6][t], 1, members) for t in range(2)]
        if inside:
            fx = [
                hll(x_lower[0], here[0], prim[7][0], 2, full),
                hll(x_lower[1], here[1], prim[7][1], 2, (XB[2, 1],)),
            ]
        else:
            fx = [hll(x_lower[0], here[0], prim[7][0], 2, (XB[2, 0],)), None]
        return fz, fy, fx

    slabs = lax.axis_size("gz") * NZ
    first_slab = lax.axis_index("gz") * NZ
    previous = None
    copies = []
    for z in range(-1, NZ + 1):
        base = 8 * (z + 1)
        prim, cen, here = slab_cells(z)
        below = previous["here"] if previous else None
        fz, fy, fx = slab_fluxes(z, prim, cen, here, below)
        now = dict(prim=prim, cen=cen, here=here, fz=fz, fy=fy, fx=fx, base=base)
        if z >= 0:
            by = [fz[t][XB[0, 1]] for t in range(2)]
            by_down = down_y(by)
            now["ex"] = [0.25 * (by[t] + by_down[t] - fy[t][XB[1, 0]] - previous["fy"][t][XB[1, 0]]) for t in range(2)]
            bx = fz[0][XB[0, 2]]
            now["ey"] = 0.25 * (fx[0][XB[2, 0]] + previous["fx"][0][XB[2, 0]] - bx - down_x(bx, col_fz, base + 3))
        if 0 <= z < NZ:
            bx = [fy[t][XB[1, 2]] for t in range(2)]
            by = [fx[t][XB[2, 1]] for t in range(2)]
            by_down = down_y(by)
            now["ez"] = [0.25 * (bx[t] + down_x(bx[t], col_fy[t], base + 3) - by[t] - by_down[t]) for t in range(2)]
        if z >= 1:
            k = z - 1
            was = previous
            cell = was["here"][0]
            pull = -GRAVITY * (2 * (first_slab + k) + 1 - slabs).astype(f32) / slabs
            squared = sum(c[0] * c[0] for c in was["cen"])
            held = [cell.rho] + cell.mom + [cell.thermal + 0.5 * squared]
            for m in range(5):
                y_next = up_y([was["fy"][t][m] for t in range(2)])[0]
                x_next = up_x(was["fx"][0][m], col_fx[0][m], was["base"] + 1)
                change = (fz[0][m] - was["fz"][0][m]) + (y_next - was["fy"][0][m]) + (x_next - was["fx"][0][m])
                value = held[m] - COURANT * change
                if m == 1:
                    value = value + (COURANT * pull) * cell.rho
                if m == 4:
                    value = value + (COURANT * pull) * cell.mom[0]
                conserved[m, k] = value
            ex, ey, ez = was["ex"], was["ey"], was["ez"]
            ex_up_y, ez_up_y = up_y(ex)[0], up_y(ez)[0]
            ey_up_x = up_x(ey, col_ey, was["base"] + 1)
            ez_up_x = up_x(ez[0], col_ez[0], was["base"] + 1)
            curls = (
                ey_up_x - ey - (ex_up_y - ex[0]),
                now["ex"][0] - ex[0] - (ez_up_x - ez[0]),
                ez_up_y - ez[0] - (now["ey"] - ey),
            )
            for c in range(3):
                faces_new[c, k] = was["prim"][5 + c][0] - COURANT * curls[c]
            for i, (here_at, there) in enumerate(((conserved, conserved_out), (faces_new, faces_out))):
                copy = pltpu.make_async_copy(here_at.at[:, k], there.at[:, k], sems.at[2 * k + i])
                copy.start()
                copies.append(copy)
        previous = now
    for copy in copies:
        copy.wait()


VMEM = pl.BlockSpec(memory_space=pltpu.VMEM)


def shape(*dims):
    return jax.ShapeDtypeStruct(dims, f32)


def held(*dims, dtype=f32):
    return pltpu.VMEM(dims, dtype)


def near(*arrays):
    return [pltpu.with_memory_space_constraint(a, pltpu.VMEM) for a in arrays]


def neighbours(axis):
    count = lax.axis_size(axis)
    return [(i, i + 1) for i in range(count - 1)], [(i + 1, i) for i in range(count - 1)]


def on_device(density, velocity, pressure, field, corona):
    anywhere = pl.BlockSpec(memory_space=pl.ANY)
    top, bottom = pl.pallas_call(
        gather_layers,
        out_shape=(held(8, NY, NX), held(9, NY, NX)),
        in_specs=[anywhere] * 4,
        out_specs=(VMEM,) * 2,
        scratch_shapes=[pltpu.SemaphoreType.DMA((9,))],
        name="gather_layers",
    )(density, velocity, pressure, field)
    up, down = neighbours("gz")
    below = lax.ppermute(top, "gz", up)
    above = lax.ppermute(bottom, "gz", down)
    own, marks = pl.pallas_call(
        gather_block,
        out_shape=(held(8, NZ, NY, NX), held(ROWS, NY, NX, dtype=jnp.int32)),
        in_specs=[anywhere] * 5,
        out_specs=(VMEM,) * 2,
        scratch_shapes=[pltpu.SMEM(corona.shape, jnp.int32), pltpu.SemaphoreType.DMA((5,))],
        name="gather_block",
    )(density, velocity, pressure, field, corona)
    rows_up, rows_down = pl.pallas_call(
        pack_rows,
        out_shape=(held(UP_ROWS, NX), held(DOWN_ROWS, NX)),
        in_specs=[VMEM] * 3,
        out_specs=(VMEM, VMEM),
        name="pack_rows",
    )(*near(own, below, above))
    up, down = neighbours("gy")
    left_rows = lax.ppermute(rows_up, "gy", up)
    right_rows = lax.ppermute(rows_down, "gy", down)
    main, main_cols = pl.pallas_call(
        pack_main,
        out_shape=(held(8, 11, 8, NX), held(3, 8, NX)),
        in_specs=[VMEM] * 4,
        out_specs=(VMEM, VMEM),
        name="pack_main",
    )(*near(marks, own, below, above))
    edges, cols = pl.pallas_call(
        pack_edges,
        out_shape=(held(8, 11, 8, NX), held(3, 16, NX)),
        in_specs=[VMEM] * 5,
        out_specs=(VMEM, VMEM),
        name="pack_edges",
    )(*near(marks, main, main_cols, left_rows, right_rows))
    gathered = lax.all_gather(cols, "gx", axis=0)
    return pl.pallas_call(
        advance,
        out_shape=(shape(5, NZ, NY, NX), shape(3, NZ, NY, NX)),
        in_specs=[VMEM] * 4,
        out_specs=(pl.BlockSpec(memory_space=pl.ANY),) * 2,
        scratch_shapes=[
            pltpu.VMEM((5, NZ, NY, NX), f32),
            pltpu.VMEM((3, NZ, NY, NX), f32),
            pltpu.SemaphoreType.DMA((2 * NZ,)),
        ],
        name="advance",
    )(*near(gathered, cols, main, edges))


def solution(mesh):
    block = P("gz", "gy", "gx")
    blocks = P(None, "gz", "gy", "gx")
    return jax.shard_map(
        on_device,
        mesh=mesh,
        in_specs=(block, blocks, block, blocks, P()),
        out_specs=(blocks, blocks),
        check_vma=False,
    )
```

```python
import jax
import jax.numpy as jnp
from jax import lax
from jax.experimental import pallas as pl
from jax.experimental.pallas import tpu as pltpu
from jax.sharding import PartitionSpec as P


COOL_STEPS = 8
GAMMA = 5.0 / 3.0
COURANT = 0.08
COOL_RATE = 0.03
GRAVITY = 1.0

NZ, NY, NX = 8, 8, 128
ROWS = 10
UP_ROWS, DOWN_ROWS = 88, 96
Z_MAIN = range(NZ)

f32 = jnp.float32


def run_copies(pairs, sems):
    copies = [pltpu.make_async_copy(a, b, sems.at[i]) for i, (a, b) in enumerate(pairs)]
    for copy in copies:
        copy.start()
    for copy in copies:
        copy.wait()


def gather_layers(density, velocity, pressure, field, top, bottom, sems):
    one = pl.ds(0, 1)
    pairs = [(field.at[0, pl.ds(1, 1)], bottom.at[pl.ds(8, 1)])]
    for out, z in ((top, NZ - 1), (bottom, 0)):
        pairs += [
            (density.at[pl.ds(z, 1)], out.at[one]),
            (velocity.at[:, z], out.at[pl.ds(1, 3)]),
            (pressure.at[pl.ds(z, 1)], out.at[pl.ds(4, 1)]),
            (field.at[:, z], out.at[pl.ds(5, 3)]),
        ]
    run_copies(pairs, sems)


def gather_block(density, velocity, pressure, field, corona, own, marks, mask, sems):
    pairs = [
        (density, own.at[0]),
        (velocity, own.at[pl.ds(1, 3)]),
        (pressure, own.at[4]),
        (field, own.at[pl.ds(5, 3)]),
        (corona, mask),
    ]
    run_copies(pairs, sems)
    first, last = lax.axis_index("gz") * NZ, lax.axis_size("gz") * NZ - 1
    for z in range(ROWS):
        marks[z] = jnp.full((8, NX), mask[jnp.clip(first + z - 1, 0, last)], jnp.int32)


def pack_rows(own, below, above, up, down):
    lowest = lax.axis_index("gz") == 0
    highest = lax.axis_index("gz") == lax.axis_size("gz") - 1

    def put(out, at, row):
        out[pl.ds(at, 1), :] = row

    for out, y in ((up, NY - 1), (down, 0)):
        for member in range(8):
            base = member * ROWS
            for z in Z_MAIN:
                put(out, base + 1 + z, own[member, z, pl.ds(y, 1), :])
            put(out, base, below[member, pl.ds(y, 1), :])
            put(out, base + 9, above[member, pl.ds(y, 1), :])
        put(out, 80, above[8, pl.ds(y, 1), :])
    for z in Z_MAIN:
        put(down, 82 + z, own[6, z, pl.ds(1, 1), :])
    put(down, 81, below[6, pl.ds(1, 1), :])
    put(down, 90, above[6, pl.ds(1, 1), :])

    @pl.when(lowest)
    def _():
        for out, y in ((up, NY - 1), (down, 0)):
            for member in range(8):
                put(out, member * ROWS, own[member, 0, pl.ds(y, 1), :])
        put(down, 81, own[6, 0, pl.ds(1, 1), :])

    @pl.when(highest)
    def _():
        for out, y in ((up, NY - 1), (down, 0)):
            for member in range(8):
                put(out, member * ROWS + 9, own[member, NZ - 1, pl.ds(y, 1), :])
            put(out, 80, own[5, NZ - 1, pl.ds(y, 1), :])
        put(down, 90, own[6, NZ - 1, pl.ds(1, 1), :])


def lanes():
    return lax.broadcasted_iota(jnp.int32, (8, NX), 1)


def sublanes():
    return lax.broadcasted_iota(jnp.int32, (8, NX), 0)


def roll(values, by, axis):
    size = values.shape[axis]
    by = by % size
    return values if by == 0 else pltpu.roll(values, by, axis)


def cool(marks, ext):
    rho = [ext[0, z] for z in range(ROWS)]
    raw = [ext[4, z] for z in range(ROWS)]
    now = list(raw)
    for _ in range(COOL_STEPS):
        now = [p / (1.0 + COOL_RATE * root(r * p)) for r, p in zip(rho, now)]
    for z, (p, q) in enumerate(zip(raw, now)):
        ext[4, z] = jnp.where(marks[z] == 1, q, p)


def columns_of(ext):
    lane = lanes()
    low = high = second = jnp.zeros((8, NX), f32)
    for z in range(11):
        for member in range(8) if z < 10 else (5,):
            at = 8 * z + member
            tile = ext[member, z]
            low = jnp.where(lane == at, roll(tile, at, 1), low)
            high = jnp.where(lane == at, roll(tile, at + 1, 1), high)
            if member == 7:
                second = jnp.where(lane == 8 * z + 2, roll(tile, 8 * z + 1, 1), second)
    return low, high, second


def pack_main(marks, own, below, above, ext, cols):
    slab_at, slab_count = lax.axis_index("gz"), lax.axis_size("gz")
    for member in range(8):
        for z in Z_MAIN:
            ext[member, z + 1] = own[member, z]
        ext[member, 0] = below[member]
        ext[member, 9] = above[member]
    ext[5, 10] = above[8]

    @pl.when(slab_at == 0)
    def _():
        for member in range(8):
            ext[member, 0] = own[member, 0]

    @pl.when(slab_at == slab_count - 1)
    def _():
        for member in range(8):
            ext[member, 9] = own[member, NZ - 1]
        ext[5, 10] = own[5, NZ - 1]

    cool(marks, ext)
    for i, v in enumerate(columns_of(ext)):
        cols[i] = v


PLACES = [(member, z, member * ROWS + z) for member in range(8) for z in range(ROWS)] + [(5, 10, 80)]


def pack_edges(marks, main, main_cols, left_rows, right_rows, ext, cols, near_out, far_out):
    row_at, row_count = lax.axis_index("gy"), lax.axis_size("gy")
    for member, z, at in PLACES:
        ext[member, z, 7:8, :] = left_rows[pl.ds(at, 1), :]
        ext[member, z, 0:1, :] = right_rows[pl.ds(at, 1), :]
    for z in range(ROWS):
        ext[6, z, 1:2, :] = right_rows[pl.ds(81 + z, 1), :]
    cool(marks, ext)

    @pl.when(row_at == 0)
    def _():
        for member, z, _at in PLACES:
            ext[member, z, 7:8, :] = main[member, z, 0:1, :]

    @pl.when(row_at == row_count - 1)
    def _():
        for member, z, _at in PLACES:
            ext[member, z, 0:1, :] = main[member, z, 7:8, :]
        for z in range(ROWS):
            ext[6, z, 1:2, :] = main[6, z, 7:8, :]

    for i, v in enumerate(columns_of(ext)):
        cols[i, 0:8, :] = main_cols[i]
        cols[i, 8:16, :] = v
    even = lax.rem(lax.axis_index("gx"), 2) == 0

    @pl.when(even)
    def _():
        near_out[0], near_out[1] = cols[1], cols[2]
        far_out[0], far_out[1] = cols[0], cols[2]

    @pl.when(jnp.logical_not(even))
    def _():
        near_out[0], near_out[1] = cols[0], cols[2]
        far_out[0], far_out[1] = cols[1], cols[2]


class Cell:
    def __init__(self, rho, vel, p, cen):
        self.rho, self.vel, self.p, self.cen = rho, vel, p, cen
        self.mom = [rho * v for v in vel]
        kinetic = self.mom[0] * vel[0] + self.mom[1] * vel[1] + self.mom[2] * vel[2]
        self.thermal = p * (1.0 / (GAMMA - 1.0)) + 0.5 * kinetic
        self.inv = 1.0 / rho
        self.sound = GAMMA * p * self.inv


def root(x):
    return x * lax.rsqrt(x)


def speeds(cell, square, axis):
    b, c = [k for k in range(3) if k != axis]
    across = cell.cen[b] * cell.cen[b] + cell.cen[c] * cell.cen[c]
    n, t, s = square * cell.inv, across * cell.inv, cell.sound
    gap = s - n - t
    inner = root(jnp.maximum(gap * gap + 4.0 * s * t, 1e-30))
    return across, root(0.5 * (s + n + t + inner))


def side(cell, normal, square, across, axis, speed, weight, member):
    vel, cen, va = cell.vel, cell.cen, cell.vel[axis]
    w, wn = weight * (va - speed), weight * normal
    if member == 0:
        return cell.rho * w
    if member == axis + 1:
        return cell.mom[axis] * w + weight * (cell.p + 0.5 * (across - square))
    if member < 4:
        return cell.mom[member - 1] * w - cen[member - 1] * wn
    b, c = [k for k in range(3) if k != axis]
    if member == 4:
        half = 0.5 * (across + square)
        align = va * normal + vel[b] * cen[b] + vel[c] * cen[c]
        return (cell.thermal + half) * w + weight * ((cell.p + half) * va - normal * align)
    k = (b, c)[member - 5]
    return cen[k] * w - vel[k] * wn


def hll(lower, upper, normal, axis, members):
    square = normal * normal
    la, lf = speeds(lower, square, axis)
    ua, uf = speeds(upper, square, axis)
    lv, uv = lower.vel[axis], upper.vel[axis]
    slow = jnp.minimum(jnp.minimum(lv - lf, uv - uf), 0.0)
    fast = jnp.maximum(jnp.maximum(lv + lf, uv + uf), 0.0)
    inverse = 1.0 / (fast - slow)
    a, b = fast * inverse, slow * inverse
    return {
        m: side(lower, normal, square, la, axis, slow, a, m) - side(upper, normal, square, ua, axis, fast, b, m)
        for m in members
    }


def member_of(axis, component):
    return 5 + [k for k in range(3) if k != axis].index(component)


def advance(near_in, far_in, own_cols, main, edges, conserved_out, faces_out, conserved, faces_new, sems):
    lane, sub = lanes(), sublanes()
    even = jnp.full((8, NX), lax.rem(lax.axis_index("gx"), 2), jnp.int32) == 0
    first_lane, last_lane = lane == 0, lane == NX - 1
    first_row, last_row = sub == 0, sub == 7
    slot = lane % 8

    def down_y(q):
        r0, r1 = roll(q[0], 1, 0), roll(q[1], 1, 0)
        return [jnp.where(first_row, r1, r0), jnp.where(first_row, r0, r1)]

    def up_y(q):
        r0, r1 = roll(q[0], -1, 0), roll(q[1], -1, 0)
        return [jnp.where(last_row, r1, r0), jnp.where(last_row, r0, r1)]

    def down_x(q, side, source):
        return jnp.where(first_lane, roll(side, -source, 1), roll(q, 1, 1))

    def up_x(q, side, source):
        return jnp.where(last_lane, roll(side, NX - 1 - source, 1), roll(q, -1, 1))

    got = lambda side, i: [side[i, 8 * t : 8 * t + 8, :] for t in range(2)]
    pick = lambda p, q: [jnp.where(even, v, w) for v, w in zip(p, q)]
    low_r = pick(got(near_in, 0), got(far_in, 0))
    two_r = pick(got(near_in, 1), got(far_in, 1))
    high_l = pick(got(far_in, 0), got(near_in, 0))
    own_low = [own_cols[0, 8 * t : 8 * t + 8, :] for t in range(2)]
    own_high = [own_cols[1, 8 * t : 8 * t + 8, :] for t in range(2)]

    def column(member):
        out = []
        for t in range(2):
            v = roll(own_high[t], -member, 1)
            v = jnp.where(slot == 1, roll(low_r[t], 1 - member, 1), v)
            v = jnp.where(slot == 3, roll(high_l[t], 3 - member, 1), v)
            v = jnp.where(slot == 4, roll(own_low[t], 4 - member, 1), v)
            if member == 7:
                v = jnp.where(slot == 2, two_r[t], v)
            out.append(v)
        return out

    col = [column(member) for member in range(8)]
    col_next_y = up_y(col[6])
    col_cen = [
        [0.5 * (v + roll(v, -8, 1)) for v in col[5]],
        [0.5 * (v + n) for v, n in zip(col[6], col_next_y)],
        [0.5 * (v + roll(v, -1, 1)) for v in col[7]],
    ]

    def cells(prim, cen):
        return [Cell(prim[0][t], [prim[k][t] for k in (1, 2, 3)], prim[4][t], [cen[k][t] for k in range(3)]) for t in range(2)]

    col_cell = cells(col, col_cen)
    shifted = lambda by: cells(
        [[roll(v, by, 1) for v in col[k]] for k in range(5)],
        [[roll(v, by, 1) for v in col_cen[k]] for k in range(3)],
    )
    full = tuple(range(7))
    col_x_lower, col_z_lower = shifted(1), shifted(8)
    col_y_lower = cells([down_y(col[k]) for k in range(5)], [down_y(col_cen[k]) for k in range(3)])
    XB = {(a, k): member_of(a, k) for a in range(3) for k in range(3) if a != k}
    col_fx = [hll(col_x_lower[0], col_cell[0], col[7][0], 2, full), hll(col_x_lower[1], col_cell[1], col[7][1], 2, (XB[2, 1],))]
    col_fy = [hll(col_y_lower[t], col_cell[t], col[6][t], 1, (XB[1, 2],))[XB[1, 2]] for t in range(2)]
    col_fz = hll(col_z_lower[0], col_cell[0], col[5][0], 0, (XB[0, 2],))[XB[0, 2]]
    fx_by = [f[XB[2, 1]] for f in col_fx]
    fx_bz = col_fx[0][XB[2, 0]]
    down = down_y(fx_by)
    col_ez = [0.25 * (col_fy[t] + roll(col_fy[t], 1, 1) - fx_by[t] - down[t]) for t in range(2)]
    col_ey = 0.25 * (fx_bz + roll(fx_bz, 8, 1) - col_fz - roll(col_fz, 1, 1))

    def slab_cells(z):
        base = 8 * (z + 1)
        get = lambda member, s: [main[member, s], edges[member, s]]
        prim = [get(member, z + 1) for member in range(8)]
        next_z = get(5, z + 2)
        next_y = up_y(prim[6])
        next_x = [up_x(prim[7][t], low_r[t], base + 7) for t in range(2)]
        cen = [
            [0.5 * (prim[5][t] + next_z[t]) for t in range(2)],
            [0.5 * (prim[6][t] + next_y[t]) for t in range(2)],
            [0.5 * (prim[7][t] + next_x[t]) for t in range(2)],
        ]
        return prim, cen, cells(prim, cen)

    def slab_fluxes(z, prim, cen, here, below):
        base = 8 * (z + 1)
        inside = 0 <= z < NZ
        fz = fy = fx = None
        if z >= 0:
            fz = [
                hll(below[0], here[0], prim[5][0], 0, full),
                hll(below[1], here[1], prim[5][1], 0, (XB[0, 1],)),
            ]
        y_lower = cells([down_y(prim[k]) for k in range(5)], [down_y(cen[k]) for k in range(3)])
        x_lower = []
        for t in range(2):
            p = [down_x(prim[k][t], high_l[t], base + k) for k in range(5)]
            c = [down_x(cen[k][t], col_cen[k][t], base + 3) for k in range(3)]
            x_lower.append(Cell(p[0], p[1:4], p[4], c))
        members = full if inside else (XB[1, 0],)
        fy = [hll(y_lower[t], here[t], prim[6][t], 1, members) for t in range(2)]
        if inside:
            fx = [
                hll(x_lower[0], here[0], prim[7][0], 2, full),
                hll(x_lower[1], here[1], prim[7][1], 2, (XB[2, 1],)),
            ]
        else:
            fx = [hll(x_lower[0], here[0], prim[7][0], 2, (XB[2, 0],)), None]
        return fz, fy, fx

    slabs = lax.axis_size("gz") * NZ
    first_slab = lax.axis_index("gz") * NZ
    previous = None
    copies = []
    for z in range(-1, NZ + 1):
        base = 8 * (z + 1)
        prim, cen, here = slab_cells(z)
        below = previous["here"] if previous else None
        fz, fy, fx = slab_fluxes(z, prim, cen, here, below)
        now = dict(prim=prim, cen=cen, here=here, fz=fz, fy=fy, fx=fx, base=base)
        if z >= 0:
            by = [fz[t][XB[0, 1]] for t in range(2)]
            by_down = down_y(by)
            now["ex"] = [0.25 * (by[t] + by_down[t] - fy[t][XB[1, 0]] - previous["fy"][t][XB[1, 0]]) for t in range(2)]
            bx = fz[0][XB[0, 2]]
            now["ey"] = 0.25 * (fx[0][XB[2, 0]] + previous["fx"][0][XB[2, 0]] - bx - down_x(bx, col_fz, base + 3))
        if 0 <= z < NZ:
            bx = [fy[t][XB[1, 2]] for t in range(2)]
            by = [fx[t][XB[2, 1]] for t in range(2)]
            by_down = down_y(by)
            now["ez"] = [0.25 * (bx[t] + down_x(bx[t], col_fy[t], base + 3) - by[t] - by_down[t]) for t in range(2)]
        if z >= 1:
            k = z - 1
            was = previous
            cell = was["here"][0]
            pull = -GRAVITY * (2 * (first_slab + k) + 1 - slabs).astype(f32) / slabs
            squared = sum(c[0] * c[0] for c in was["cen"])
            held = [cell.rho] + cell.mom + [cell.thermal + 0.5 * squared]
            for m in range(5):
                y_next = up_y([was["fy"][t][m] for t in range(2)])[0]
                x_next = up_x(was["fx"][0][m], col_fx[0][m], was["base"] + 1)
                change = (fz[0][m] - was["fz"][0][m]) + (y_next - was["fy"][0][m]) + (x_next - was["fx"][0][m])
                value = held[m] - COURANT * change
                if m == 1:
                    value = value + (COURANT * pull) * cell.rho
                if m == 4:
                    value = value + (COURANT * pull) * cell.mom[0]
                conserved[m, k] = value
            ex, ey, ez = was["ex"], was["ey"], was["ez"]
            ex_up_y, ez_up_y = up_y(ex)[0], up_y(ez)[0]
            ey_up_x = up_x(ey, col_ey, was["base"] + 1)
            ez_up_x = up_x(ez[0], col_ez[0], was["base"] + 1)
            curls = (
                ey_up_x - ey - (ex_up_y - ex[0]),
                now["ex"][0] - ex[0] - (ez_up_x - ez[0]),
                ez_up_y - ez[0] - (now["ey"] - ey),
            )
            for c in range(3):
                faces_new[c, k] = was["prim"][5 + c][0] - COURANT * curls[c]
            for i, (here_at, there) in enumerate(((conserved, conserved_out), (faces_new, faces_out))):
                copy = pltpu.make_async_copy(here_at.at[:, k], there.at[:, k], sems.at[2 * k + i])
                copy.start()
                copies.append(copy)
        previous = now
    for copy in copies:
        copy.wait()


VMEM = pl.BlockSpec(memory_space=pltpu.VMEM)


def shape(*dims):
    return jax.ShapeDtypeStruct(dims, f32)


def held(*dims, dtype=f32):
    return pltpu.VMEM(dims, dtype)


def near(*arrays):
    return [pltpu.with_memory_space_constraint(a, pltpu.VMEM) for a in arrays]


def neighbours(axis):
    count = lax.axis_size(axis)
    return [(i, i + 1) for i in range(count - 1)], [(i + 1, i) for i in range(count - 1)]


def on_device(density, velocity, pressure, field, corona):
    anywhere = pl.BlockSpec(memory_space=pl.ANY)
    top, bottom = pl.pallas_call(
        gather_layers,
        out_shape=(held(8, NY, NX), held(9, NY, NX)),
        in_specs=[anywhere] * 4,
        out_specs=(VMEM,) * 2,
        scratch_shapes=[pltpu.SemaphoreType.DMA((9,))],
        name="gather_layers",
    )(density, velocity, pressure, field)
    up, down = neighbours("gz")
    below = lax.ppermute(top, "gz", up)
    above = lax.ppermute(bottom, "gz", down)
    own, marks = pl.pallas_call(
        gather_block,
        out_shape=(held(8, NZ, NY, NX), held(ROWS, NY, NX, dtype=jnp.int32)),
        in_specs=[anywhere] * 5,
        out_specs=(VMEM,) * 2,
        scratch_shapes=[pltpu.SMEM(corona.shape, jnp.int32), pltpu.SemaphoreType.DMA((5,))],
        name="gather_block",
    )(density, velocity, pressure, field, corona)
    rows_up, rows_down = pl.pallas_call(
        pack_rows,
        out_shape=(held(UP_ROWS, NX), held(DOWN_ROWS, NX)),
        in_specs=[VMEM] * 3,
        out_specs=(VMEM, VMEM),
        name="pack_rows",
    )(*near(own, below, above))
    up, down = neighbours("gy")
    left_rows = lax.ppermute(rows_up, "gy", up)
    right_rows = lax.ppermute(rows_down, "gy", down)
    main, main_cols = pl.pallas_call(
        pack_main,
        out_shape=(held(8, 11, 8, NX), held(3, 8, NX)),
        in_specs=[VMEM] * 4,
        out_specs=(VMEM, VMEM),
        name="pack_main",
    )(*near(marks, own, below, above))
    edges, cols, to_near, to_far = pl.pallas_call(
        pack_edges,
        out_shape=(held(8, 11, 8, NX), held(3, 16, NX), held(2, 16, NX), held(2, 16, NX)),
        in_specs=[VMEM] * 5,
        out_specs=(VMEM,) * 4,
        name="pack_edges",
    )(*near(marks, main, main_cols, left_rows, right_rows))
    count = lax.axis_size("gx")
    near_pairs = [(i, i ^ 1) for i in range(count)]
    far_pairs = [p for i in range(1, count, 2) for p in ((i, (i + 1) % count), ((i + 1) % count, i))]
    from_far = lax.ppermute(to_far, "gx", far_pairs)
    from_near = lax.ppermute(to_near, "gx", near_pairs)
    return pl.pallas_call(
        advance,
        out_shape=(shape(5, NZ, NY, NX), shape(3, NZ, NY, NX)),
        in_specs=[VMEM] * 5,
        out_specs=(pl.BlockSpec(memory_space=pl.ANY),) * 2,
        scratch_shapes=[
            pltpu.VMEM((5, NZ, NY, NX), f32),
            pltpu.VMEM((3, NZ, NY, NX), f32),
            pltpu.SemaphoreType.DMA((2 * NZ,)),
        ],
        name="advance",
    )(*near(from_near, from_far, cols, main, edges))


def solution(mesh):
    block = P("gz", "gy", "gx")
    blocks = P(None, "gz", "gy", "gx")
    return jax.shard_map(
        on_device,
        mesh=mesh,
        in_specs=(block, blocks, block, blocks, P()),
        out_specs=(blocks, blocks),
        check_vma=False,
    )
```
